512 devices in a mesh: group: 32 (over z, y_hi), proc: 16 (over y_lo, x, core).
Axes of the slice: x: 4, y: 8 (y_hi: 4, y_lo: 2; y = y_hi * 2 + y_lo), z: 8, core: 2. Of those that a mesh axis runs over, the one named last changes fastest.
Arguments:
- ancestor_rows: bfloat16 [32, 256, 8192], P('group', 'proc'), may hold values from -6 to 6
- piece_owner: int32 [32], replicated, may hold values from 0 to 31, each once
- structure: int32 [32, 8], replicated, may hold values from 0 to 15, as said below
- kept_blocks: int32 [32, 7], replicated, may hold values from 0 to 7, as said below
- panel_parent: bfloat16 [32, 8, 2, 256, 512], P('group', None, None, 'proc'), may hold values from -0.09375 to 0.09375
- panel_child: bfloat16 [32, 8, 2, 256, 512], P('group', None, None, 'proc'), may hold values from -0.09375 to 0.09375
- pivot_parent: bfloat16 [32, 2, 256, 512], P('group', None, 'proc'), may hold values from -4 to 6, as said below
- pivot_child: bfloat16 [32, 2, 256, 512], P('group', None, 'proc'), may hold values from -4 to 6, as said below
Outputs:
- column_parent: bfloat16 [32, 8, 2, 256, 512], P('group', None, None, 'proc')
- block_parent: bfloat16 [32, 2, 256, 512], P('group', None, 'proc')
- column_child: bfloat16 [32, 8, 2, 256, 512], P('group', None, None, 'proc')
- block_child: bfloat16 [32, 2, 256, 512], P('group', None, 'proc')
The draws below stay inside these ranges and needn't reach their ends.
Inputs may be any that keep to these rules, and one draw needn't show every extreme that they name: `structure`: each row names 8 different top supernodes in increasing order. `kept_blocks`: each row names 7 different positions in increasing order. `piece_owner`: a permutation. `pivot_parent`: each group's block, read as a 512 x 512 matrix, is symmetric. `pivot_child`: each group's block, read as a 512 x 512 matrix, is symmetric.
All inputs are finite; a program needn't handle non-finite values.
Results may differ from the reference program's by a relative error of at most 0.018.
Values may be sent and summed in bfloat16 or wider, within the bound.
No kernel may reach another device: no remote copies, remote signals or barrier semaphores. Data moves between devices by JAX's collectives and lax.ppermute only.
A program may use at most 64 MiB of HBM per device.

```python
import jax
import jax.numpy as jnp
from jax import lax

W = 512
RB = 8
NT = 16
PIECES = 2
GROUPS = 32


def draw_structure(key, part):
    heat_key, noise_key = jax.random.split(jax.random.fold_in(key, 101))
    heat = jax.random.randint(heat_key, (NT,), 0, 4)
    noise = jax.random.randint(noise_key, (GROUPS, NT), 0, 6)
    score = (noise + 3 * heat[None, :]) * NT + jnp.arange(NT)[None, :]
    chosen = lax.top_k(score, RB)[1]
    return jnp.sort(chosen, axis=1).astype(jnp.int32)


def draw_kept_blocks(key, part):
    dropped = jax.random.randint(jax.random.fold_in(key, 202), (GROUPS, 1), 0, RB)
    positions = jnp.arange(RB - 1)[None, :]
    return (positions + (positions >= dropped).astype(jnp.int32)).astype(jnp.int32)


def symmetric_pivot(key):
    sample = jnp.clip(jax.random.normal(key, (GROUPS, W, W), jnp.float32), -4.0, 4.0)
    symmetric = 0.5 * (sample + jnp.swapaxes(sample, 1, 2)) + 2.0 * jnp.eye(W, dtype=jnp.float32)[None]
    return symmetric.reshape(GROUPS, PIECES, W // PIECES, W).astype(jnp.bfloat16)


def draw_pivot_parent(key, part):
    return symmetric_pivot(jax.random.fold_in(key, 303))


def draw_pivot_child(key, part):
    return symmetric_pivot(jax.random.fold_in(key, 404))


def block_levels(stream_key, dims, pieces, least, largest):
    gain, own = 1.0, jax.random.fold_in(stream_key, 6)
    for dim, blocks in pieces:
        draws = jnp.exp(jax.random.uniform(jax.random.fold_in(own, dim), (blocks,), jnp.float32, least / len(pieces), largest / len(pieces)))
        gain = gain * jnp.repeat(draws, dims[dim] // blocks).reshape([-1 if axis == dim else 1 for axis in range(len(dims))])
    return gain


def normal_values(key, shape, scale, limit, pieces=(), kind=jnp.bfloat16):
    loudness = block_levels(key, shape, pieces, -0.22, 0.18) if pieces else 1.0
    drawn = jax.random.normal(key, shape, jnp.float32) * scale * loudness
    return jnp.minimum(jnp.maximum(drawn, -limit), limit).astype(kind)


def setup_inputs(seed: int = 0) -> dict:
    arg_keys = jax.random.split(jax.random.key(seed), 9)
    return {
        "ancestor_rows": normal_values(arg_keys[0], (NT * PIECES, W // PIECES, NT * W), 1.0, 6.0, ((0, 32), (1, 16))),
        "piece_owner": jax.random.permutation(arg_keys[1], NT * PIECES).astype(jnp.int32),
        "structure": draw_structure(jax.random.fold_in(arg_keys[8], 71), 0),
        "kept_blocks": draw_kept_blocks(jax.random.fold_in(arg_keys[8], 71), 0),
        "panel_parent": normal_values(arg_keys[4], (GROUPS, RB, PIECES, W // PIECES, W), (RB * W) ** -0.5, 0.09375, ((0, 32), (3, 16))),
        "panel_child": normal_values(arg_keys[5], (GROUPS, RB, PIECES, W // PIECES, W), (RB * W) ** -0.5, 0.09375, ((0, 32), (3, 16))),
        "pivot_parent": draw_pivot_parent(jax.random.fold_in(arg_keys[8], 71), 0),
        "pivot_child": draw_pivot_child(jax.random.fold_in(arg_keys[8], 71), 0),
    }


def product(left_side, right_side):
    return jnp.dot(left_side, right_side, preferred_element_type=jnp.float32, precision=lax.Precision.HIGHEST)


def reference(ancestor_rows, piece_owner, structure, kept_blocks, panel_parent, panel_child, pivot_parent, pivot_child):
    ancestor = ancestor_rows[piece_owner].reshape(NT, W, NT, W)
    order = RB * W

    def per_group(inputs):
        own_structure, kept_positions, first_panel, second_panel, first_pivot, second_pivot = inputs
        upper = ancestor[own_structure][:, :, own_structure, :].astype(jnp.float32).reshape(order, order)
        lower_first = first_panel.astype(jnp.float32).reshape(order, W)
        column_first = (-product(upper, lower_first)).astype(jnp.bfloat16)
        block_first = (first_pivot.astype(jnp.float32).reshape(W, W) - product(lower_first.T, column_first.astype(jnp.float32))).astype(jnp.bfloat16)
        stacked = jnp.concatenate([block_first[None], column_first.reshape(RB, W, W)[kept_positions]], axis=0).astype(jnp.float32)
        lower_second = second_panel.astype(jnp.float32).reshape(order, W)
        first_rows = product(stacked.reshape(order, W).T, lower_second)
        inner = upper.reshape(RB, W, RB, W)[kept_positions][:, :, kept_positions, :].reshape((RB - 1) * W, (RB - 1) * W)
        other_rows = product(stacked[1:].reshape((RB - 1) * W, W), lower_second[:W]) + product(inner, lower_second[W:])
        column_second = (-jnp.concatenate([first_rows, other_rows], axis=0)).astype(jnp.bfloat16)
        block_second = (second_pivot.astype(jnp.float32).reshape(W, W) - product(lower_second.T, column_second.astype(jnp.float32))).astype(jnp.bfloat16)
        return (column_first.reshape(RB, PIECES, W // PIECES, W), block_first.reshape(PIECES, W // PIECES, W),
                column_second.reshape(RB, PIECES, W // PIECES, W), block_second.reshape(PIECES, W // PIECES, W))

    results = lax.map(per_group, (structure, kept_blocks, panel_parent, panel_child, pivot_parent, pivot_child))
    return (results[0], results[1], results[2], results[3])
```

```python
import jax
import jax.numpy as jnp
from jax import lax
from jax.experimental import pallas as pl
from jax.experimental.pallas import tpu as pltpu
from jax.sharding import PartitionSpec as P

INTERPRET = False
F32 = jnp.float32
BF16 = jnp.bfloat16


def dot(a, b):
    return jnp.dot(a, b, preferred_element_type=F32)


def dot_rows(a, b):
    return lax.dot_general(a, b, (((0,), (0,)), ((), ())), preferred_element_type=F32)


def products_kernel(kept, upper, panels, own_first, own_second, pivot, column_out, child_out, sums_out):
    strip, pieces, blocks, slabs, half = upper.shape
    procs, width = panels.shape[0], panels.shape[-1]
    rows = strip * slabs

    def left(h, b):
        return upper[:, h, b].reshape(rows, half)

    def right(n, b, h):
        return panels[:, n, b, h].reshape(half, width)

    total = jnp.zeros((rows, width), F32)
    for b in range(blocks):
        for h in range(pieces):
            total += dot(left(h, b), right(0, b, h))
    column = (-total).astype(BF16)
    at = lax.broadcasted_iota(jnp.int32, (rows, rows), 0)
    of = lax.broadcasted_iota(jnp.int32, (rows, rows), 1)
    same_row = (at % strip == of // slabs) & ((at // strip) % pieces == of % pieces)
    to_block = at // (strip * pieces)
    of_block = (of % slabs) // pieces
    wanted = jnp.full((rows, rows), -1, jnp.int32)
    for b in range(1, blocks):
        wanted = jnp.where(to_block == b, kept[b - 1], wanted)
    in_order = (same_row & (to_block == of_block)).astype(F32).astype(BF16)
    in_child = (same_row & (wanted == of_block)).astype(F32).astype(BF16)
    column_natural = dot(in_order, column).astype(BF16)
    column_kept = dot(in_child, column).astype(BF16)
    column_out[...] = column_natural.reshape(column_out.shape)

    top = [right(1, 0, h) for h in range(pieces)]
    total = jnp.zeros((rows, width), F32)
    for b in range(1, blocks):
        for h in range(pieces):
            total += dot(left(h, kept[b - 1]), right(1, b, h))
    for h in range(pieces):
        total += dot(column[:, h * half : (h + 1) * half], top[h])
    child = dot(in_child, (-total).astype(BF16)).astype(BF16)
    child_out[...] = child.reshape(child_out.shape)

    first = own_first[...].reshape(rows, width)
    second = own_second[...].reshape(rows, width)
    diagonal = pivot[...].reshape(strip * pieces, width)
    parent_sum = dot_rows(first, column_natural)
    cross = jnp.zeros((rows, width), F32)
    for h in range(pieces):
        cross += dot(first[:, h * half : (h + 1) * half], top[h])
    head_sum = (
        dot_rows(column_kept, second)
        - dot_rows(column_natural, cross.astype(BF16))
        + dot_rows(diagonal, second[: strip * pieces])
    ).astype(BF16)
    child_sum = -dot_rows(second, child)
    for h in range(pieces):
        child_sum += dot_rows(top[h], head_sum[h * half : (h + 1) * half])
    for n, value in enumerate((parent_sum.astype(BF16), head_sum, child_sum.astype(BF16))):
        for h in range(pieces):
            for p in range(procs):
                start = h * half + p * strip
                sums_out[p, n, h] = value[start : start + strip]


def final_kernel(arrived, pivot_first, pivot_second, child_in, block_first, child_out, block_second):
    del child_in
    sums = [arrived[0, n].astype(F32) for n in range(3)]
    for p in range(1, arrived.shape[0]):
        for n in range(3):
            sums[n] += arrived[p, n].astype(F32)
    block_first[...] = (pivot_first[...].astype(F32) - sums[0]).astype(BF16)
    child_out[0] = (-sums[1]).astype(BF16)
    block_second[...] = (pivot_second[...].astype(F32) + sums[2]).astype(BF16)


def per_device(
    ancestor_rows,
    piece_owner,
    structure,
    kept_blocks,
    panel_parent,
    panel_child,
    pivot_parent,
    pivot_child,
):
    group_index = lax.axis_index("group")
    strip = ancestor_rows.shape[1]
    groups, blocks = structure.shape
    procs = lax.axis_size("proc")
    pieces = panel_parent.shape[2]
    width = panel_parent.shape[-1]
    half = width // pieces
    tops = ancestor_rows.shape[2] // width
    slabs = blocks * pieces

    panels = lax.all_gather(jnp.stack([panel_parent[0], panel_child[0]]), "proc", axis=0)

    spread = ancestor_rows.reshape(strip, tops, pieces, half).transpose(0, 2, 1, 3)
    spread = lax.all_to_all(
        spread.reshape(groups, tops, half), "group", split_axis=0, concat_axis=0, tiled=True
    )
    wanted = structure[:, :, None] * pieces + jnp.arange(pieces, dtype=jnp.int32)
    owner = piece_owner[wanted.reshape(groups, slabs)]
    index = owner[:, None, :] * tops + structure[:, :, None]
    choice = jax.nn.one_hot(index.reshape(-1), groups * tops, dtype=BF16)
    outgoing = jnp.dot(choice, spread.reshape(groups * tops, half), preferred_element_type=BF16)
    upper = lax.all_to_all(
        outgoing.reshape(groups, blocks, slabs, half), "group", split_axis=0, concat_axis=0, tiled=True
    ).reshape(strip, pieces, blocks, slabs, half)

    vmem = pl.BlockSpec(memory_space=pltpu.VMEM)
    column_parent, column_child, sums = pl.pallas_call(
        products_kernel,
        out_shape=(
            jax.ShapeDtypeStruct((blocks, pieces, strip, width), BF16),
            jax.ShapeDtypeStruct((blocks, pieces, strip, width), BF16),
            jax.ShapeDtypeStruct((procs, 3, pieces, strip, width), BF16),
        ),
        in_specs=[pl.BlockSpec(memory_space=pltpu.SMEM)] + [vmem] * 5,
        out_specs=(vmem, vmem, vmem),
        interpret=INTERPRET,
        name="products",
    )(kept_blocks[group_index], upper, panels, panel_parent[0], panel_child[0], pivot_parent[0])
    arrived = lax.all_to_all(sums, "proc", split_axis=0, concat_axis=0, tiled=True)
    whole = pl.BlockSpec((pieces, strip, width), lambda i: (0, 0, 0))
    block_parent, column_child, block_child = pl.pallas_call(
        final_kernel,
        grid=(1,),
        out_shape=(
            jax.ShapeDtypeStruct((pieces, strip, width), BF16),
            jax.ShapeDtypeStruct((blocks, pieces, strip, width), BF16),
            jax.ShapeDtypeStruct((pieces, strip, width), BF16),
        ),
        in_specs=[
            pl.BlockSpec(arrived.shape, lambda i: (0, 0, 0, 0, 0)),
            whole,
            whole,
            pl.BlockSpec(memory_space=pl.ANY),
        ],
        out_specs=(whole, pl.BlockSpec((1, pieces, strip, width), lambda i: (0, 0, 0, 0)), whole),
        input_output_aliases={3: 1},
        interpret=INTERPRET,
        name="final",
    )(arrived, pivot_parent[0], pivot_child[0], column_child)
    return column_parent[None], block_parent[None], column_child[None], block_child[None]


def solution(mesh):
    in_specs = (
        P("group", "proc", None),
        P(),
        P(),
        P(),
        P("group", None, None, "proc", None),
        P("group", None, None, "proc", None),
        P("group", None, "proc", None),
        P("group", None, "proc", None),
    )
    out_specs = (
        P("group", None, None, "proc", None),
        P("group", None, "proc", None),
        P("group", None, None, "proc", None),
        P("group", None, "proc", None),
    )
    return jax.shard_map(
        per_device, mesh=mesh, in_specs=in_specs, out_specs=out_specs, check_vma=False
    )
```

```python
import jax
import jax.numpy as jnp
from jax import lax
from jax.experimental import pallas as pl
from jax.experimental.pallas import tpu as pltpu
from jax.sharding import PartitionSpec as P


INTERPRET = False
YS, XS, CORES = 2, 4, 2
PROCS = YS * XS * CORES
F32 = jnp.float32
BF16 = jnp.bfloat16


def dot(a, b):
    return jnp.dot(a, b, preferred_element_type=F32)


def dot_rows(a, b):
    return lax.dot_general(a, b, (((0,), (0,)), ((), ())), preferred_element_type=F32)


def products_kernel(kept, upper, mine, theirs, own_first, own_second, pivot, column_out, child_out, sums_out):
    strip, pieces, blocks, slabs, half = upper.shape
    procs, width = CORES * mine.shape[0], mine.shape[-1]
    first_core = kept[blocks - 1] == 0
    rows = strip * slabs

    def left(h, b):
        return upper[:, h, b].reshape(rows, half)

    def right(n, b, h):
        a, b = mine[:, n, b, h], theirs[:, n, b, h]
        pair = jnp.stack([jnp.where(first_core, a, b), jnp.where(first_core, b, a)], axis=1)
        return pair.reshape(half, width)

    total = jnp.zeros((rows, width), F32)
    for b in range(blocks):
        for h in range(pieces):
            total += dot(left(h, b), right(0, b, h))
    column = (-total).astype(BF16)
    at = lax.broadcasted_iota(jnp.int32, (rows, rows), 0)
    of = lax.broadcasted_iota(jnp.int32, (rows, rows), 1)
    same_row = (at % strip == of // slabs) & ((at // strip) % pieces == of % pieces)
    to_block = at // (strip * pieces)
    of_block = (of % slabs) // pieces
    wanted = jnp.full((rows, rows), -1, jnp.int32)
    for b in range(1, blocks):
        wanted = jnp.where(to_block == b, kept[b - 1], wanted)
    in_order = (same_row & (to_block == of_block)).astype(F32).astype(BF16)
    in_child = (same_row & (wanted == of_block)).astype(F32).astype(BF16)
    column_natural = dot(in_order, column).astype(BF16)
    column_kept = dot(in_child, column).astype(BF16)
    column_out[...] = column_natural.reshape(column_out.shape)

    top = [right(1, 0, h) for h in range(pieces)]
    total = jnp.zeros((rows, width), F32)
    for b in range(1, blocks):
        for h in range(pieces):
            total += dot(left(h, kept[b - 1]), right(1, b, h))
    for h in range(pieces):
        total += dot(column[:, h * half : (h + 1) * half], top[h])
    child = dot(in_child, (-total).astype(BF16)).astype(BF16)
    child_out[...] = child.reshape(child_out.shape)

    first = own_first[...].reshape(rows, width)
    second = own_second[...].reshape(rows, width)
    diagonal = pivot[...].reshape(strip * pieces, width)
    parent_sum = dot_rows(first, column_natural)
    cross = jnp.zeros((rows, width), F32)
    for h in range(pieces):
        cross += dot(first[:, h * half : (h + 1) * half], top[h])
    head_sum = (
        dot_rows(column_kept, second)
        - dot_rows(column_natural, cross.astype(BF16))
        + dot_rows(diagonal, second[: strip * pieces])
    ).astype(BF16)
    child_sum = -dot_rows(second, child)
    for h in range(pieces):
        child_sum += dot_rows(top[h], head_sum[h * half : (h + 1) * half])
    for n, value in enumerate((parent_sum.astype(BF16), head_sum, child_sum.astype(BF16))):
        for h in range(pieces):
            for p in range(procs):
                start = h * half + p * strip
                sums_out[p, n, h] = value[start : start + strip]


def final_kernel(arrived, pivot_first, pivot_second, child_in, block_first, child_out, block_second):
    del child_in
    sums = [arrived[0, n].astype(F32) for n in range(3)]
    for p in range(1, arrived.shape[0]):
        for n in range(3):
            sums[n] += arrived[p, n].astype(F32)
    block_first[...] = (pivot_first[...].astype(F32) - sums[0]).astype(BF16)
    child_out[0] = (-sums[1]).astype(BF16)
    block_second[...] = (pivot_second[...].astype(F32) + sums[2]).astype(BF16)


def moved(value, step):
    pairs = []
    for p in range(PROCS):
        y, x, core = p // (XS * CORES), p // CORES % XS, p % CORES
        y, x, core = (y + step[0]) % YS, (x + step[1]) % XS, (core + step[2]) % CORES
        pairs.append((p, (y * XS + x) * CORES + core))
    return lax.ppermute(value, "proc", pairs)


def placed(buffer, value, where):
    return lax.dynamic_update_slice(buffer, value, tuple(where) + (0,) * (buffer.ndim - len(where)))


def shifted(shard):
    here = lax.axis_index("proc")
    y, x = here >> 3, (here >> 1) & (XS - 1)
    other = moved(shard, (1, 0, 0))
    parts = []
    for dy, part in ((0, shard), (1, other)):
        for dx in range(XS):
            arrived = moved(part, (0, dx, 0)) if dx else part
            parts.append((arrived, ((y + dy) & (YS - 1), (x - dx) & (XS - 1))))
    return parts


def gathered(parts, start):
    for part, where in parts:
        start = placed(start, part[None, None], where)
    other_core = moved(start, (0, 0, 1))
    shape = (YS * XS,) + start.shape[2:]
    return start.reshape(shape), other_core.reshape(shape)


def per_device(
    ancestor_rows,
    piece_owner,
    structure,
    kept_blocks,
    panel_parent,
    panel_child,
    pivot_parent,
    pivot_child,
):
    group_index = lax.axis_index("group")
    strip = ancestor_rows.shape[1]
    groups, blocks = structure.shape
    procs = lax.axis_size("proc")
    pieces = panel_parent.shape[2]
    width = panel_parent.shape[-1]
    half = width // pieces
    tops = ancestor_rows.shape[2] // width
    slabs = blocks * pieces

    parts = shifted(jnp.stack([panel_parent[0], panel_child[0]]))

    spread = ancestor_rows.reshape(strip, tops, pieces, half).transpose(0, 2, 1, 3)
    spread = lax.all_to_all(
        spread.reshape(groups, tops, half), "group", split_axis=0, concat_axis=0, tiled=True
    )
    wanted = structure[:, :, None] * pieces + jnp.arange(pieces, dtype=jnp.int32)
    owner = piece_owner[wanted.reshape(groups, slabs)]
    index = owner[:, None, :] * tops + structure[:, :, None]
    choice = jax.nn.one_hot(index.reshape(-1), groups * tops, dtype=BF16)
    outgoing = jnp.dot(choice, spread.reshape(groups * tops, half), preferred_element_type=BF16)
    start = jnp.zeros((YS, XS) + parts[0][0].shape, BF16)
    outgoing, start = lax.optimization_barrier((outgoing, start))
    mine, theirs = gathered(parts, start)
    upper = lax.all_to_all(
        outgoing.reshape(groups, blocks, slabs, half), "group", split_axis=0, concat_axis=0, tiled=True
    )
    upper = upper.reshape(strip, pieces, blocks, slabs, half)

    core = lax.axis_index("proc") & (CORES - 1)
    scalars = jnp.concatenate([kept_blocks[group_index], core[None].astype(jnp.int32)])
    vmem = pl.BlockSpec(memory_space=pltpu.VMEM)
    column_parent, column_child, sums = pl.pallas_call(
        products_kernel,
        out_shape=(
            jax.ShapeDtypeStruct((blocks, pieces, strip, width), BF16),
            jax.ShapeDtypeStruct((blocks, pieces, strip, width), BF16),
            jax.ShapeDtypeStruct((procs, 3, pieces, strip, width), BF16),
        ),
        in_specs=[pl.BlockSpec(memory_space=pltpu.SMEM)] + [vmem] * 6,
        out_specs=(vmem, vmem, vmem),
        compiler_params=pltpu.CompilerParams(vmem_limit_bytes=32 * 1024 * 1024),
        interpret=INTERPRET,
        name="products",
    )(scalars, upper, mine, theirs, panel_parent[0], panel_child[0], pivot_parent[0])
    arrived = lax.all_to_all(sums, "proc", split_axis=0, concat_axis=0, tiled=True)
    whole = pl.BlockSpec((pieces, strip, width), lambda i: (0, 0, 0))
    block_parent, column_child, block_child = pl.pallas_call(
        final_kernel,
        grid=(1,),
        out_shape=(
            jax.ShapeDtypeStruct((pieces, strip, width), BF16),
            jax.ShapeDtypeStruct((blocks, pieces, strip, width), BF16),
            jax.ShapeDtypeStruct((pieces, strip, width), BF16),
        ),
        in_specs=[
            pl.BlockSpec(arrived.shape, lambda i: (0, 0, 0, 0, 0)),
            whole,
            whole,
            pl.BlockSpec(memory_space=pl.ANY),
        ],
        out_specs=(whole, pl.BlockSpec((1, pieces, strip, width), lambda i: (0, 0, 0, 0)), whole),
        input_output_aliases={3: 1},
        interpret=INTERPRET,
        name="final",
    )(arrived, pivot_parent[0], pivot_child[0], column_child)
    return column_parent[None], block_parent[None], column_child[None], block_child[None]


def solution(mesh):
    in_specs = (
        P("group", "proc", None),
        P(),
        P(),
        P(),
        P("group", None, None, "proc", None),
        P("group", None, None, "proc", None),
        P("group", None, "proc", None),
        P("group", None, "proc", None),
    )
    out_specs = (
        P("group", None, None, "proc", None),
        P("group", None, "proc", None),
        P("group", None, None, "proc", None),
        P("group", None, "proc", None),
    )

    return jax.shard_map(per_device, mesh=mesh, in_specs=in_specs, out_specs=out_specs, check_vma=False)
```

```python
import jax
import jax.numpy as jnp
from jax import lax
from jax.experimental import pallas as pl
from jax.experimental.pallas import tpu as pltpu
from jax.sharding import PartitionSpec as P


INTERPRET = False
YS, XS, CORES = 2, 4, 2
PROCS = YS * XS * CORES
F32 = jnp.float32
BF16 = jnp.bfloat16


def dot(a, b):
    return jnp.dot(a, b, preferred_element_type=F32)


def dot_rows(a, b):
    return lax.dot_general(a, b, (((0,), (0,)), ((), ())), preferred_element_type=F32)


def products_kernel(
    kept, upper, mine, theirs, own_first, own_second, pivot, column_out, child_out, sums_out, panels, sems
):
    strip, pieces, blocks, slabs, half = upper.shape
    procs, width = PROCS, panels.shape[-1]
    rows = strip * slabs
    core = kept[blocks - 1]
    order = [(1, 0)] + [(0, b) for b in range(blocks)] + [(1, b) for b in range(1, blocks)]
    copies = {}
    for n, b in order:
        copies[n, b] = [
            pltpu.make_async_copy(mine.at[:, n, b], panels.at[:, core, n, b], sems.at[n, b, 0]),
            pltpu.make_async_copy(theirs.at[:, n, b], panels.at[:, 1 - core, n, b], sems.at[n, b, 1]),
        ]
        for copy in copies[n, b]:
            copy.start()

    def left(h, b):
        return upper[:, h, b].reshape(rows, half)

    def right(n, b, h):
        return panels[:, :, n, b, h].reshape(half, width)

    def arrive(n, b):
        for copy in copies[n, b]:
            copy.wait()

    arrive(1, 0)
    total = jnp.zeros((rows, width), F32)
    for b in range(blocks):
        arrive(0, b)
        for h in range(pieces):
            total += dot(left(h, b), right(0, b, h))
    column = (-total).astype(BF16)
    at = lax.broadcasted_iota(jnp.int32, (rows, rows), 0)
    of = lax.broadcasted_iota(jnp.int32, (rows, rows), 1)
    same_row = (at % strip == of // slabs) & ((at // strip) % pieces == of % pieces)
    to_block = at // (strip * pieces)
    of_block = (of % slabs) // pieces
    wanted = jnp.full((rows, rows), -1, jnp.int32)
    for b in range(1, blocks):
        wanted = jnp.where(to_block == b, kept[b - 1], wanted)
    in_order = (same_row & (to_block == of_block)).astype(F32).astype(BF16)
    in_child = (same_row & (wanted == of_block)).astype(F32).astype(BF16)
    column_natural = dot(in_order, column).astype(BF16)
    column_kept = dot(in_child, column).astype(BF16)
    column_out[...] = column_natural.reshape(column_out.shape)

    top = [right(1, 0, h) for h in range(pieces)]
    total = jnp.zeros((rows, width), F32)
    for b in range(1, blocks):
        arrive(1, b)
        for h in range(pieces):
            total += dot(left(h, kept[b - 1]), right(1, b, h))
    for h in range(pieces):
        total += dot(column[:, h * half : (h + 1) * half], top[h])
    child = dot(in_child, (-total).astype(BF16)).astype(BF16)
    child_out[...] = child.reshape(child_out.shape)

    first = own_first[...].reshape(rows, width)
    second = own_second[...].reshape(rows, width)
    diagonal = pivot[...].reshape(strip * pieces, width)
    parent_sum = dot_rows(first, column_natural)
    cross = jnp.zeros((rows, width), F32)
    for h in range(pieces):
        cross += dot(first[:, h * half : (h + 1) * half], top[h])
    head_sum = (
        dot_rows(column_kept, second)
        - dot_rows(column_natural, cross.astype(BF16))
        + dot_rows(diagonal, second[: strip * pieces])
    ).astype(BF16)
    child_sum = -dot_rows(second, child)
    for h in range(pieces):
        child_sum += dot_rows(top[h], head_sum[h * half : (h + 1) * half])
    for n, value in enumerate((parent_sum.astype(BF16), head_sum, child_sum.astype(BF16))):
        for h in range(pieces):
            for p in range(procs):
                start = h * half + p * strip
                sums_out[p, n, h] = value[start : start + strip]


def final_kernel(arrived, pivot_first, pivot_second, child_in, block_first, child_out, block_second):
    del child_in
    sums = [arrived[0, n].astype(F32) for n in range(3)]
    for p in range(1, arrived.shape[0]):
        for n in range(3):
            sums[n] += arrived[p, n].astype(F32)
    block_first[...] = (pivot_first[...].astype(F32) - sums[0]).astype(BF16)
    child_out[0] = (-sums[1]).astype(BF16)
    block_second[...] = (pivot_second[...].astype(F32) + sums[2]).astype(BF16)


def moved(value, step):
    pairs = []
    for p in range(PROCS):
        y, x, core = p // (XS * CORES), p // CORES % XS, p % CORES
        y, x, core = (y + step[0]) % YS, (x + step[1]) % XS, (core + step[2]) % CORES
        pairs.append((p, (y * XS + x) * CORES + core))
    return lax.ppermute(value, "proc", pairs)


def placed(buffer, value, where):
    return lax.dynamic_update_slice(buffer, value, tuple(where) + (0,) * (buffer.ndim - len(where)))


def shifted(shard):
    here = lax.axis_index("proc")
    y, x = here >> 3, (here >> 1) & (XS - 1)
    other = moved(shard, (1, 0, 0))
    parts = []
    for dy, part in ((0, shard), (1, other)):
        for dx in range(XS):
            arrived = moved(part, (0, dx, 0)) if dx else part
            parts.append((arrived, ((y + dy) & (YS - 1), (x - dx) & (XS - 1))))
    return parts


def gathered(parts, start):
    for part, where in parts:
        start = placed(start, part[None, None], where)
    other_core = moved(start, (0, 0, 1))
    shape = (YS * XS,) + start.shape[2:]
    return start.reshape(shape), other_core.reshape(shape)


def per_device(
    ancestor_rows,
    piece_owner,
    structure,
    kept_blocks,
    panel_parent,
    panel_child,
    pivot_parent,
    pivot_child,
):
    group_index = lax.axis_index("group")
    strip = ancestor_rows.shape[1]
    groups, blocks = structure.shape
    procs = lax.axis_size("proc")
    pieces = panel_parent.shape[2]
    width = panel_parent.shape[-1]
    half = width // pieces
    tops = ancestor_rows.shape[2] // width
    slabs = blocks * pieces

    parts = shifted(jnp.stack([panel_parent[0], panel_child[0]]))

    spread = ancestor_rows.reshape(strip, tops, pieces, half).transpose(0, 2, 1, 3)
    spread = lax.all_to_all(
        spread.reshape(groups, tops, half), "group", split_axis=0, concat_axis=0, tiled=True
    )
    owners = piece_owner.reshape(tops, pieces)
    same = structure[:, :, None, None] == jnp.arange(tops, dtype=jnp.int32)[:, None]
    owner = jnp.where(same, owners, 0).sum(axis=2).reshape(groups, slabs)
    index = owner[:, None, :] * tops + structure[:, :, None]
    choice = jax.nn.one_hot(index.reshape(-1), groups * tops, dtype=BF16)
    outgoing = jnp.dot(choice, spread.reshape(groups * tops, half), preferred_element_type=BF16)
    start = jnp.zeros((YS, XS) + parts[0][0].shape, BF16)
    outgoing, start = lax.optimization_barrier((outgoing, start))
    mine, theirs = gathered(parts, start)
    upper = lax.all_to_all(
        outgoing.reshape(groups, blocks, slabs, half), "group", split_axis=0, concat_axis=0, tiled=True
    )
    upper = upper.reshape(strip, pieces, blocks, slabs, half)

    core = lax.axis_index("proc") & (CORES - 1)
    scalars = jnp.concatenate([kept_blocks[group_index], core[None].astype(jnp.int32)])
    smem = pl.BlockSpec(memory_space=pltpu.SMEM)
    vmem = pl.BlockSpec(memory_space=pltpu.VMEM)
    anywhere = pl.BlockSpec(memory_space=pl.ANY)
    column_parent, column_child, sums = pl.pallas_call(
        products_kernel,
        out_shape=(
            jax.ShapeDtypeStruct((blocks, pieces, strip, width), BF16),
            jax.ShapeDtypeStruct((blocks, pieces, strip, width), BF16),
            jax.ShapeDtypeStruct((procs, 3, pieces, strip, width), BF16),
        ),
        in_specs=[smem, vmem, anywhere, anywhere, vmem, vmem, vmem],
        out_specs=(vmem, vmem, vmem),
        scratch_shapes=[
            pltpu.VMEM(mine.shape[:1] + (CORES,) + mine.shape[1:], BF16),
            pltpu.SemaphoreType.DMA((2, blocks, 2)),
        ],
        compiler_params=pltpu.CompilerParams(vmem_limit_bytes=32 * 1024 * 1024),
        interpret=INTERPRET,
        name="products",
    )(scalars, upper, mine, theirs, panel_parent[0], panel_child[0], pivot_parent[0])
    arrived = lax.all_to_all(sums, "proc", split_axis=0, concat_axis=0, tiled=True)
    whole = pl.BlockSpec((pieces, strip, width), lambda i: (0, 0, 0))
    block_parent, column_child, block_child = pl.pallas_call(
        final_kernel,
        grid=(1,),
        out_shape=(
            jax.ShapeDtypeStruct((pieces, strip, width), BF16),
            jax.ShapeDtypeStruct((blocks, pieces, strip, width), BF16),
            jax.ShapeDtypeStruct((pieces, strip, width), BF16),
        ),
        in_specs=[
            pl.BlockSpec(arrived.shape, lambda i: (0, 0, 0, 0, 0)),
            whole,
            whole,
            pl.BlockSpec(memory_space=pl.ANY),
        ],
        out_specs=(whole, pl.BlockSpec((1, pieces, strip, width), lambda i: (0, 0, 0, 0)), whole),
        input_output_aliases={3: 1},
        interpret=INTERPRET,
        name="final",
    )(arrived, pivot_parent[0], pivot_child[0], column_child)
    return column_parent[None], block_parent[None], column_child[None], block_child[None]


def solution(mesh):
    in_specs = (
        P("group", "proc", None),
        P(),
        P(),
        P(),
        P("group", None, None, "proc", None),
        P("group", None, None, "proc", None),
        P("group", None, "proc", None),
        P("group", None, "proc", None),
    )
    out_specs = (
        P("group", None, None, "proc", None),
        P("group", None, "proc", None),
        P("group", None, None, "proc", None),
        P("group", None, "proc", None),
    )

    return jax.shard_map(per_device, mesh=mesh, in_specs=in_specs, out_specs=out_specs, check_vma=False)
```

```python
import jax
import jax.numpy as jnp
from jax import lax
from jax.experimental import pallas as pl
from jax.experimental.pallas import tpu as pltpu
from jax.sharding import PartitionSpec as P


INTERPRET = False
YS, XS, CORES = 2, 4, 2
PROCS = YS * XS * CORES
F32 = jnp.float32
BF16 = jnp.bfloat16


def dot(a, b):
    return jnp.dot(a, b, preferred_element_type=F32)


def dot_rows(a, b):
    return lax.dot_general(a, b, (((0,), (0,)), ((), ())), preferred_element_type=F32)


def products_kernel(
    kept, upper, mine, theirs, own_first, own_second, pivot, column_out, child_out, keep_out, give_out, panels, sems
):
    strip, pieces, blocks, slabs, half = upper.shape
    procs, width = PROCS, panels.shape[-1]
    rows = strip * slabs
    core = kept[blocks - 1]
    order = [(1, 0)] + [(0, b) for b in range(blocks)] + [(1, b) for b in range(1, blocks)]
    copies = {}
    for n, b in order:
        copies[n, b] = [
            pltpu.make_async_copy(mine.at[:, n, b], panels.at[:, core, n, b], sems.at[n, b, 0]),
            pltpu.make_async_copy(theirs.at[:, n, b], panels.at[:, 1 - core, n, b], sems.at[n, b, 1]),
        ]
        for copy in copies[n, b]:
            copy.start()

    def left(h, b):
        return upper[:, h, b].reshape(rows, half)

    def right(n, b, h):
        return panels[:, :, n, b, h].reshape(half, width)

    def arrive(n, b):
        for copy in copies[n, b]:
            copy.wait()

    arrive(1, 0)
    total = jnp.zeros((rows, width), F32)
    for b in range(blocks):
        arrive(0, b)
        for h in range(pieces):
            total += dot(left(h, b), right(0, b, h))
    column = (-total).astype(BF16)
    at = lax.broadcasted_iota(jnp.int32, (rows, rows), 0)
    of = lax.broadcasted_iota(jnp.int32, (rows, rows), 1)
    same_row = (at % strip == of // slabs) & ((at // strip) % pieces == of % pieces)
    to_block = at // (strip * pieces)
    of_block = (of % slabs) // pieces
    wanted = jnp.full((rows, rows), -1, jnp.int32)
    for b in range(1, blocks):
        wanted = jnp.where(to_block == b, kept[b - 1], wanted)
    in_order = (same_row & (to_block == of_block)).astype(F32).astype(BF16)
    in_child = (same_row & (wanted == of_block)).astype(F32).astype(BF16)
    column_natural = dot(in_order, column).astype(BF16)
    column_kept = dot(in_child, column).astype(BF16)
    column_out[...] = column_natural.reshape(column_out.shape)

    top = [right(1, 0, h) for h in range(pieces)]
    total = jnp.zeros((rows, width), F32)
    for b in range(1, blocks):
        arrive(1, b)
        for h in range(pieces):
            total += dot(left(h, kept[b - 1]), right(1, b, h))
    for h in range(pieces):
        total += dot(column[:, h * half : (h + 1) * half], top[h])
    child = dot(in_child, (-total).astype(BF16)).astype(BF16)
    child_out[...] = child.reshape(child_out.shape)

    first = own_first[...].reshape(rows, width)
    second = own_second[...].reshape(rows, width)
    diagonal = pivot[...].reshape(strip * pieces, width)
    parent_sum = dot_rows(first, column_natural)
    cross = jnp.zeros((rows, width), F32)
    for h in range(pieces):
        cross += dot(first[:, h * half : (h + 1) * half], top[h])
    head_sum = (
        dot_rows(column_kept, second)
        - dot_rows(column_natural, cross.astype(BF16))
        + dot_rows(diagonal, second[: strip * pieces])
    ).astype(BF16)
    child_sum = -dot_rows(second, child)
    for h in range(pieces):
        child_sum += dot_rows(top[h], head_sum[h * half : (h + 1) * half])
    for n, value in enumerate((parent_sum.astype(BF16), head_sum, child_sum.astype(BF16))):
        for h in range(pieces):
            for place in range(procs // CORES):
                start = h * half + place * CORES * strip
                a, b = value[start : start + strip], value[start + strip : start + CORES * strip]
                keep_out[place, n, h] = jnp.where(core == 0, a, b)
                give_out[place, n, h] = jnp.where(core == 0, b, a)


def final_kernel(arrived, pivot_first, pivot_second, child_in, block_first, child_out, block_second):
    del child_in
    sums = [arrived[0, n].astype(F32) for n in range(3)]
    for p in range(1, arrived.shape[0]):
        for n in range(3):
            sums[n] += arrived[p, n].astype(F32)
    block_first[...] = (pivot_first[...].astype(F32) - sums[0]).astype(BF16)
    child_out[0] = (-sums[1]).astype(BF16)
    block_second[...] = (pivot_second[...].astype(F32) + sums[2]).astype(BF16)


def moved(value, step):
    pairs = []
    for p in range(PROCS):
        y, x, core = p // (XS * CORES), p // CORES % XS, p % CORES
        y, x, core = (y + step[0]) % YS, (x + step[1]) % XS, (core + step[2]) % CORES
        pairs.append((p, (y * XS + x) * CORES + core))
    return lax.ppermute(value, "proc", pairs)


def placed(buffer, value, where):
    return lax.dynamic_update_slice(buffer, value, tuple(where) + (0,) * (buffer.ndim - len(where)))


def shifted(shard):
    here = lax.axis_index("proc")
    y, x = here >> 3, (here >> 1) & (XS - 1)
    other = moved(shard, (1, 0, 0))
    parts = []
    for dy, part in ((0, shard), (1, other)):
        for dx in range(XS):
            arrived = moved(part, (0, dx, 0)) if dx else part
            parts.append((arrived, ((y + dy) & (YS - 1), (x - dx) & (XS - 1))))
    return parts


def gathered(parts, start):
    for part, where in parts:
        start = placed(start, part[None, None], where)
    other_core = moved(start, (0, 0, 1))
    shape = (YS * XS,) + start.shape[2:]
    return start.reshape(shape), other_core.reshape(shape)


def per_device(
    ancestor_rows,
    piece_owner,
    structure,
    kept_blocks,
    panel_parent,
    panel_child,
    pivot_parent,
    pivot_child,
):
    group_index = lax.axis_index("group")
    strip = ancestor_rows.shape[1]
    groups, blocks = structure.shape
    procs = lax.axis_size("proc")
    pieces = panel_parent.shape[2]
    width = panel_parent.shape[-1]
    half = width // pieces
    tops = ancestor_rows.shape[2] // width
    slabs = blocks * pieces

    parts = shifted(jnp.stack([panel_parent[0], panel_child[0]]))

    spread = ancestor_rows.reshape(strip, tops, pieces, half).transpose(0, 2, 1, 3)
    spread = lax.all_to_all(
        spread.reshape(groups, tops, half), "group", split_axis=0, concat_axis=0, tiled=True
    )
    owners = piece_owner.reshape(tops, pieces)
    same = structure[:, :, None, None] == jnp.arange(tops, dtype=jnp.int32)[:, None]
    owner = jnp.where(same, owners, 0).sum(axis=2).reshape(groups, slabs)
    index = owner[:, None, :] * tops + structure[:, :, None]
    choice = jax.nn.one_hot(index.reshape(-1), groups * tops, dtype=BF16)
    outgoing = jnp.dot(choice, spread.reshape(groups * tops, half), preferred_element_type=BF16)
    start = jnp.zeros((YS, XS) + parts[0][0].shape, BF16)
    outgoing, start = lax.optimization_barrier((outgoing, start))
    mine, theirs = gathered(parts, start)
    upper = lax.all_to_all(
        outgoing.reshape(groups, blocks, slabs, half), "group", split_axis=0, concat_axis=0, tiled=True
    )
    upper = upper.reshape(strip, pieces, blocks, slabs, half)

    core = lax.axis_index("proc") & (CORES - 1)
    scalars = jnp.concatenate([kept_blocks[group_index], core[None].astype(jnp.int32)])
    smem = pl.BlockSpec(memory_space=pltpu.SMEM)
    vmem = pl.BlockSpec(memory_space=pltpu.VMEM)
    anywhere = pl.BlockSpec(memory_space=pl.ANY)
    column_parent, column_child, keep, give = pl.pallas_call(
        products_kernel,
        out_shape=(
            jax.ShapeDtypeStruct((blocks, pieces, strip, width), BF16),
            jax.ShapeDtypeStruct((blocks, pieces, strip, width), BF16),
            jax.ShapeDtypeStruct((procs // CORES, 3, pieces, strip, width), BF16),
            jax.ShapeDtypeStruct((procs // CORES, 3, pieces, strip, width), BF16),
        ),
        in_specs=[smem, vmem, anywhere, anywhere, vmem, vmem, vmem],
        out_specs=(vmem, vmem, vmem, vmem),
        scratch_shapes=[
            pltpu.VMEM(mine.shape[:1] + (CORES,) + mine.shape[1:], BF16),
            pltpu.SemaphoreType.DMA((2, blocks, 2)),
        ],
        compiler_params=pltpu.CompilerParams(vmem_limit_bytes=32 * 1024 * 1024),
        interpret=INTERPRET,
        name="products",
    )(scalars, upper, mine, theirs, panel_parent[0], panel_child[0], pivot_parent[0])
    sums = (keep.astype(F32) + moved(give, (0, 0, 1)).astype(F32)).astype(BF16)
    same_core = [[place * CORES + c for place in range(procs // CORES)] for c in range(CORES)]
    arrived = lax.all_to_all(
        sums, "proc", split_axis=0, concat_axis=0, tiled=True, axis_index_groups=same_core
    )
    whole = pl.BlockSpec((pieces, strip, width), lambda i: (0, 0, 0))
    block_parent, column_child, block_child = pl.pallas_call(
        final_kernel,
        grid=(1,),
        out_shape=(
            jax.ShapeDtypeStruct((pieces, strip, width), BF16),
            jax.ShapeDtypeStruct((blocks, pieces, strip, width), BF16),
            jax.ShapeDtypeStruct((pieces, strip, width), BF16),
        ),
        in_specs=[
            pl.BlockSpec(arrived.shape, lambda i: (0, 0, 0, 0, 0)),
            whole,
            whole,
            pl.BlockSpec(memory_space=pl.ANY),
        ],
        out_specs=(whole, pl.BlockSpec((1, pieces, strip, width), lambda i: (0, 0, 0, 0)), whole),
        input_output_aliases={3: 1},
        interpret=INTERPRET,
        name="final",
    )(arrived, pivot_parent[0], pivot_child[0], column_child)
    return column_parent[None], block_parent[None], column_child[None], block_child[None]


def solution(mesh):
    in_specs = (
        P("group", "proc", None),
        P(),
        P(),
        P(),
        P("group", None, None, "proc", None),
        P("group", None, None, "proc", None),
        P("group", None, "proc", None),
        P("group", None, "proc", None),
    )
    out_specs = (
        P("group", None, None, "proc", None),
        P("group", None, "proc", None),
        P("group", None, None, "proc", None),
        P("group", None, "proc", None),
    )

    return jax.shard_map(per_device, mesh=mesh, in_specs=in_specs, out_specs=out_specs, check_vma=False)
```

```python
import jax
import jax.numpy as jnp
from jax import lax
from jax.experimental import pallas as pl
from jax.experimental.pallas import tpu as pltpu
from jax.sharding import PartitionSpec as P


INTERPRET = False
YS, XS, CORES = 2, 4, 2
PROCS = YS * XS * CORES
F32 = jnp.float32
BF16 = jnp.bfloat16


def dot(a, b):
    return jnp.dot(a, b, preferred_element_type=F32)


def dot_rows(a, b):
    return lax.dot_general(a, b, (((0,), (0,)), ((), ())), preferred_element_type=F32)


def products_kernel(
    kept, received, near, near_other, far, far_other, own_first, own_second, pivot, column_out, child_out, keep_out, give_out, upper, panels, sems, upper_sems
):
    strip, pieces, blocks, slabs, half = upper.shape
    procs, width = PROCS, panels.shape[-1]
    rows = strip * slabs
    core, y = kept[blocks - 1], kept[blocks]
    sources = ((near, y, core), (near_other, y, 1 - core), (far, 1 - y, core), (far_other, 1 - y, 1 - core))
    order = [(1, 0)] + [(0, b) for b in range(blocks)] + [(1, b) for b in range(1, blocks)]
    copies = {}
    for n, b in order:
        copies[n, b] = [
            pltpu.make_async_copy(source.at[:, n, b], panels.at[at_y, :, at_core, n, b], sems.at[n, b, k])
            for k, (source, at_y, at_core) in enumerate(sources)
        ]
        if n == 0:
            copies[n, b].append(pltpu.make_async_copy(received.at[:, :, b], upper.at[:, :, b], upper_sems.at[b]))
        for copy in copies[n, b]:
            copy.start()

    def left(h, b):
        return upper[:, h, b].reshape(rows, half)

    def right(n, b, h):
        return panels[:, :, :, n, b, h].reshape(half, width)

    def arrive(n, b):
        for copy in copies[n, b]:
            copy.wait()

    arrive(1, 0)
    total = jnp.zeros((rows, width), F32)
    for b in range(blocks):
        arrive(0, b)
        for h in range(pieces):
            total += dot(left(h, b), right(0, b, h))
    column = (-total).astype(BF16)
    at = lax.broadcasted_iota(jnp.int32, (rows, rows), 0)
    of = lax.broadcasted_iota(jnp.int32, (rows, rows), 1)
    same_row = (at % strip == of // slabs) & ((at // strip) % pieces == of % pieces)
    to_block = at // (strip * pieces)
    of_block = (of % slabs) // pieces
    wanted = jnp.full((rows, rows), -1, jnp.int32)
    for b in range(1, blocks):
        wanted = jnp.where(to_block == b, kept[b - 1], wanted)
    in_order = (same_row & (to_block == of_block)).astype(F32).astype(BF16)
    in_child = (same_row & (wanted == of_block)).astype(F32).astype(BF16)
    column_natural = dot(in_order, column).astype(BF16)
    column_kept = dot(in_child, column).astype(BF16)
    column_out[...] = column_natural.reshape(column_out.shape)

    top = [right(1, 0, h) for h in range(pieces)]
    first = own_first[...].reshape(rows, width)
    second = own_second[...].reshape(rows, width)
    diagonal = pivot[...].reshape(strip * pieces, width)
    parent_sum = dot_rows(first, column_natural)
    cross = jnp.zeros((rows, width), F32)
    for h in range(pieces):
        cross += dot(first[:, h * half : (h + 1) * half], top[h])
    head_sum = (
        dot_rows(column_kept, second)
        - dot_rows(column_natural, cross.astype(BF16))
        + dot_rows(diagonal, second[: strip * pieces])
    ).astype(BF16)
    child_sum = jnp.zeros((width, width), F32)
    for h in range(pieces):
        child_sum += dot_rows(top[h], head_sum[h * half : (h + 1) * half])

    total = jnp.zeros((rows, width), F32)
    for b in range(1, blocks):
        arrive(1, b)
        for h in range(pieces):
            total += dot(left(h, kept[b - 1]), right(1, b, h))
    for h in range(pieces):
        total += dot(column[:, h * half : (h + 1) * half], top[h])
    child = dot(in_child, (-total).astype(BF16)).astype(BF16)
    child_out[...] = child.reshape(child_out.shape)
    child_sum -= dot_rows(second, child)
    for n, value in enumerate((parent_sum.astype(BF16), head_sum, child_sum.astype(BF16))):
        for h in range(pieces):
            for place in range(procs // CORES):
                start = h * half + place * CORES * strip
                a, b = value[start : start + strip], value[start + strip : start + CORES * strip]
                keep_out[place, n, h] = jnp.where(core == 0, a, b)
                give_out[place, n, h] = jnp.where(core == 0, b, a)


def final_kernel(arrived, pivot_first, pivot_second, child_in, block_first, child_out, block_second):
    del child_in
    sums = [arrived[0, n].astype(F32) for n in range(3)]
    for p in range(1, arrived.shape[0]):
        for n in range(3):
            sums[n] += arrived[p, n].astype(F32)
    block_first[...] = (pivot_first[...].astype(F32) - sums[0]).astype(BF16)
    child_out[0] = (-sums[1]).astype(BF16)
    block_second[...] = (pivot_second[...].astype(F32) + sums[2]).astype(BF16)


def moved(value, step):
    pairs = []
    for p in range(PROCS):
        y, x, core = p // (XS * CORES), p // CORES % XS, p % CORES
        y, x, core = (y + step[0]) % YS, (x + step[1]) % XS, (core + step[2]) % CORES
        pairs.append((p, (y * XS + x) * CORES + core))
    return lax.ppermute(value, "proc", pairs)


def placed(buffer, value, where):
    return lax.dynamic_update_slice(buffer, value, tuple(where) + (0,) * (buffer.ndim - len(where)))


def shifted(shard):
    x = (lax.axis_index("proc") >> 1) & (XS - 1)
    other = moved(shard, (1, 0, 0))
    rows = []
    for part in (shard, other):
        row = [(part, x)]
        for dx in range(1, XS):
            row.append((moved(part, (0, dx, 0)), (x - dx) & (XS - 1)))
        rows.append(row)
    return rows


def gathered(rows, starts):
    both = []
    for row, start in zip(rows, starts):
        for part, x in row:
            start = placed(start, part[None], (x,))
        both += [start, moved(start, (0, 0, 1))]
    return both


def per_device(
    ancestor_rows,
    piece_owner,
    structure,
    kept_blocks,
    panel_parent,
    panel_child,
    pivot_parent,
    pivot_child,
):
    group_index = lax.axis_index("group")
    strip = ancestor_rows.shape[1]
    groups, blocks = structure.shape
    procs = lax.axis_size("proc")
    pieces = panel_parent.shape[2]
    width = panel_parent.shape[-1]
    half = width // pieces
    tops = ancestor_rows.shape[2] // width
    slabs = blocks * pieces

    rows = shifted(jnp.stack([panel_parent[0], panel_child[0]]))

    spread = ancestor_rows.reshape(strip, tops, pieces, half).transpose(0, 2, 1, 3)
    spread = lax.all_to_all(
        spread.reshape(groups, tops, half), "group", split_axis=0, concat_axis=0, tiled=True
    )
    owners = piece_owner.reshape(tops, pieces)
    same = structure[:, :, None, None] == jnp.arange(tops, dtype=jnp.int32)[:, None]
    owner = jnp.where(same, owners, 0).sum(axis=2).reshape(groups, slabs)
    index = owner[:, None, :] * tops + structure[:, :, None]
    choice = jax.nn.one_hot(index.reshape(-1), groups * tops, dtype=BF16)
    outgoing = jnp.dot(choice, spread.reshape(groups * tops, half), preferred_element_type=BF16)
    panels_shape = (XS, 2) + panel_parent.shape[1:]
    starts = [jnp.zeros(panels_shape, BF16) for _ in range(YS)]
    outgoing, starts = lax.optimization_barrier((outgoing, starts))
    gathered_panels = gathered(rows, starts)
    upper = lax.all_to_all(
        outgoing.reshape(groups, blocks, slabs, half), "group", split_axis=0, concat_axis=0, tiled=True
    )
    upper = upper.reshape(strip, pieces, blocks, slabs, half)

    here = lax.axis_index("proc")
    place = jnp.stack([here & (CORES - 1), here >> 3]).astype(jnp.int32)
    scalars = jnp.concatenate([kept_blocks[group_index], place])
    smem = pl.BlockSpec(memory_space=pltpu.SMEM)
    vmem = pl.BlockSpec(memory_space=pltpu.VMEM)
    anywhere = pl.BlockSpec(memory_space=pl.ANY)
    column_parent, column_child, keep, give = pl.pallas_call(
        products_kernel,
        out_shape=(
            jax.ShapeDtypeStruct((blocks, pieces, strip, width), BF16),
            jax.ShapeDtypeStruct((blocks, pieces, strip, width), BF16),
            jax.ShapeDtypeStruct((procs // CORES, 3, pieces, strip, width), BF16),
            jax.ShapeDtypeStruct((procs // CORES, 3, pieces, strip, width), BF16),
        ),
        in_specs=[smem] + [anywhere] * 5 + [vmem] * 3,
        out_specs=(vmem, vmem, vmem, vmem),
        scratch_shapes=[
            pltpu.VMEM(upper.shape, BF16),
            pltpu.VMEM((YS, XS, CORES) + panels_shape[1:], BF16),
            pltpu.SemaphoreType.DMA((2, blocks, 4)),
            pltpu.SemaphoreType.DMA((blocks,)),
        ],
        compiler_params=pltpu.CompilerParams(vmem_limit_bytes=32 * 1024 * 1024),
        interpret=INTERPRET,
        name="products",
    )(scalars, upper, *gathered_panels, panel_parent[0], panel_child[0], pivot_parent[0])
    sums = (keep.astype(F32) + moved(give, (0, 0, 1)).astype(F32)).astype(BF16)
    same_core = [[place * CORES + c for place in range(procs // CORES)] for c in range(CORES)]
    arrived = lax.all_to_all(
        sums, "proc", split_axis=0, concat_axis=0, tiled=True, axis_index_groups=same_core
    )
    whole = pl.BlockSpec((pieces, strip, width), lambda i: (0, 0, 0))
    block_parent, column_child, block_child = pl.pallas_call(
        final_kernel,
        grid=(1,),
        out_shape=(
            jax.ShapeDtypeStruct((pieces, strip, width), BF16),
            jax.ShapeDtypeStruct((blocks, pieces, strip, width), BF16),
            jax.ShapeDtypeStruct((pieces, strip, width), BF16),
        ),
        in_specs=[
            pl.BlockSpec(arrived.shape, lambda i: (0, 0, 0, 0, 0)),
            whole,
            whole,
            pl.BlockSpec(memory_space=pl.ANY),
        ],
        out_specs=(whole, pl.BlockSpec((1, pieces, strip, width), lambda i: (0, 0, 0, 0)), whole),
        input_output_aliases={3: 1},
        interpret=INTERPRET,
        name="final",
    )(arrived, pivot_parent[0], pivot_child[0], column_child)
    return column_parent[None], block_parent[None], column_child[None], block_child[None]


def solution(mesh):
    in_specs = (
        P("group", "proc", None),
        P(),
        P(),
        P(),
        P("group", None, None, "proc", None),
        P("group", None, None, "proc", None),
        P("group", None, "proc", None),
        P("group", None, "proc", None),
    )
    out_specs = (
        P("group", None, None, "proc", None),
        P("group", None, "proc", None),
        P("group", None, None, "proc", None),
        P("group", None, "proc", None),
    )

    return jax.shard_map(per_device, mesh=mesh, in_specs=in_specs, out_specs=out_specs, check_vma=False)
```

```python
import jax
import jax.numpy as jnp
from jax import lax
from jax.experimental import pallas as pl
from jax.experimental.pallas import tpu as pltpu
from jax.sharding import PartitionSpec as P


INTERPRET = False
YS, XS, CORES = 2, 4, 2
PROCS = YS * XS * CORES
F32 = jnp.float32
BF16 = jnp.bfloat16


def dot(a, b):
    return jnp.dot(a, b, preferred_element_type=F32)


def dot_rows(a, b):
    return lax.dot_general(a, b, (((0,), (0,)), ((), ())), preferred_element_type=F32)


def products_kernel(
    kept, upper, near, near_other, far, far_other, own_first, own_second, pivot, column_out, child_out, keep_out, give_out, panels, sems
):
    strip, pieces, blocks, slabs, half = upper.shape
    procs, width = PROCS, panels.shape[-1]
    rows = strip * slabs
    core, y = kept[blocks - 1], kept[blocks]
    sources = ((near, y, core), (near_other, y, 1 - core), (far, 1 - y, core), (far_other, 1 - y, 1 - core))
    order = [(1, 0)] + [(0, b) for b in range(blocks)] + [(1, b) for b in range(1, blocks)]
    copies = {}
    for n, b in order:
        copies[n, b] = [
            pltpu.make_async_copy(source.at[:, n, b], panels.at[at_y, :, at_core, n, b], sems.at[n, b, k])
            for k, (source, at_y, at_core) in enumerate(sources)
        ]
        for copy in copies[n, b]:
            copy.start()

    def left(h, b):
        return upper[:, h, b].reshape(rows, half)

    def right(n, b, h):
        return panels[:, :, :, n, b, h].reshape(half, width)

    def arrive(n, b):
        for copy in copies[n, b]:
            copy.wait()

    arrive(1, 0)
    total = jnp.zeros((rows, width), F32)
    for b in range(blocks):
        arrive(0, b)
        for h in range(pieces):
            total += dot(left(h, b), right(0, b, h))
    column = (-total).astype(BF16)
    at = lax.broadcasted_iota(jnp.int32, (rows, rows), 0)
    of = lax.broadcasted_iota(jnp.int32, (rows, rows), 1)
    same_row = (at % strip == of // slabs) & ((at // strip) % pieces == of % pieces)
    to_block = at // (strip * pieces)
    of_block = (of % slabs) // pieces
    wanted = jnp.full((rows, rows), -1, jnp.int32)
    for b in range(1, blocks):
        wanted = jnp.where(to_block == b, kept[b - 1], wanted)
    in_order = (same_row & (to_block == of_block)).astype(F32).astype(BF16)
    in_child = (same_row & (wanted == of_block)).astype(F32).astype(BF16)
    column_natural = dot(in_order, column).astype(BF16)
    column_kept = dot(in_child, column).astype(BF16)
    column_out[...] = column_natural.reshape(column_out.shape)

    top = [right(1, 0, h) for h in range(pieces)]
    first = own_first[...].reshape(rows, width)
    second = own_second[...].reshape(rows, width)
    diagonal = pivot[...].reshape(strip * pieces, width)
    parent_sum = dot_rows(first, column_natural)
    cross = jnp.zeros((rows, width), F32)
    for h in range(pieces):
        cross += dot(first[:, h * half : (h + 1) * half], top[h])
    head_sum = (
        dot_rows(column_kept, second)
        - dot_rows(column_natural, cross.astype(BF16))
        + dot_rows(diagonal, second[: strip * pieces])
    ).astype(BF16)
    child_sum = jnp.zeros((width, width), F32)
    for h in range(pieces):
        child_sum += dot_rows(top[h], head_sum[h * half : (h + 1) * half])

    total = jnp.zeros((rows, width), F32)
    for b in range(1, blocks):
        arrive(1, b)
        for h in range(pieces):
            total += dot(left(h, kept[b - 1]), right(1, b, h))
    for h in range(pieces):
        total += dot(column[:, h * half : (h + 1) * half], top[h])
    child = dot(in_child, (-total).astype(BF16)).astype(BF16)
    child_out[...] = child.reshape(child_out.shape)
    child_sum -= dot_rows(second, child)
    for n, value in enumerate((parent_sum.astype(BF16), head_sum, child_sum.astype(BF16))):
        for h in range(pieces):
            for place in range(procs // CORES):
                start = h * half + place * CORES * strip
                a, b = value[start : start + strip], value[start + strip : start + CORES * strip]
                keep_out[place, n, h] = jnp.where(core == 0, a, b)
                give_out[place, n, h] = jnp.where(core == 0, b, a)


def final_kernel(arrived, pivot_first, pivot_second, child_in, block_first, child_out, block_second):
    del child_in
    sums = [arrived[0, n].astype(F32) for n in range(3)]
    for p in range(1, arrived.shape[0]):
        for n in range(3):
            sums[n] += arrived[p, n].astype(F32)
    block_first[...] = (pivot_first[...].astype(F32) - sums[0]).astype(BF16)
    child_out[0] = (-sums[1]).astype(BF16)
    block_second[...] = (pivot_second[...].astype(F32) + sums[2]).astype(BF16)


def moved(value, step):
    pairs = []
    for p in range(PROCS):
        y, x, core = p // (XS * CORES), p // CORES % XS, p % CORES
        y, x, core = (y + step[0]) % YS, (x + step[1]) % XS, (core + step[2]) % CORES
        pairs.append((p, (y * XS + x) * CORES + core))
    return lax.ppermute(value, "proc", pairs)


def assemble_kernel(place, *refs):
    parts, out, sems = refs[:XS], refs[XS], refs[XS + 1]
    copies = [
        pltpu.make_async_copy(part, out.at[(place[0] - dx) & (XS - 1)], sems.at[dx])
        for dx, part in enumerate(parts)
    ]
    for copy in copies:
        copy.start()
    for copy in copies:
        copy.wait()


def shifted(shard):
    other = moved(shard, (1, 0, 0))
    rows = []
    for part in (shard, other):
        row = [part]
        for dx in range(1, XS):
            row.append(moved(part, (0, dx, 0)))
        rows.append(row)
    return rows


def gathered(rows):
    place = ((lax.axis_index("proc") >> 1) & (XS - 1))[None].astype(jnp.int32)
    anywhere = pl.BlockSpec(memory_space=pl.ANY)
    both = []
    for row in rows:
        together = pl.pallas_call(
            assemble_kernel,
            out_shape=pltpu.HBM((XS,) + row[0].shape, BF16),
            in_specs=[pl.BlockSpec(memory_space=pltpu.SMEM)] + [anywhere] * XS,
            out_specs=pl.BlockSpec(memory_space=pltpu.HBM),
            scratch_shapes=[pltpu.SemaphoreType.DMA((XS,))],
            interpret=INTERPRET,
            name="assemble",
        )(place, *row)
        pair = [together, moved(together, (0, 0, 1))]
        both += [pltpu.with_memory_space_constraint(half, pltpu.HBM) for half in pair]
    return both


def per_device(
    ancestor_rows,
    piece_owner,
    structure,
    kept_blocks,
    panel_parent,
    panel_child,
    pivot_parent,
    pivot_child,
):
    group_index = lax.axis_index("group")
    strip = ancestor_rows.shape[1]
    groups, blocks = structure.shape
    procs = lax.axis_size("proc")
    pieces = panel_parent.shape[2]
    width = panel_parent.shape[-1]
    half = width // pieces
    tops = ancestor_rows.shape[2] // width
    slabs = blocks * pieces

    rows = shifted(jnp.stack([panel_parent[0], panel_child[0]]))

    spread = ancestor_rows.reshape(strip, tops, pieces, half).transpose(0, 2, 1, 3)
    spread = lax.all_to_all(
        spread.reshape(groups, tops, half), "group", split_axis=0, concat_axis=0, tiled=True
    )
    owners = piece_owner.reshape(tops, pieces)
    same = structure[:, :, None, None] == jnp.arange(tops, dtype=jnp.int32)[:, None]
    owner = jnp.where(same, owners, 0).sum(axis=2).reshape(groups, slabs)
    index = owner[:, None, :] * tops + structure[:, :, None]
    choice = jax.nn.one_hot(index.reshape(-1), groups * tops, dtype=BF16)
    outgoing = jnp.dot(choice, spread.reshape(groups * tops, half), preferred_element_type=BF16)
    panels_shape = (XS, 2) + panel_parent.shape[1:]
    gathered_panels = gathered(rows)
    upper = lax.all_to_all(
        outgoing.reshape(groups, blocks, slabs, half), "group", split_axis=0, concat_axis=0, tiled=True
    )
    upper = upper.reshape(strip, pieces, blocks, slabs, half)

    here = lax.axis_index("proc")
    place = jnp.stack([here & (CORES - 1), here >> 3]).astype(jnp.int32)
    scalars = jnp.concatenate([kept_blocks[group_index], place])
    smem = pl.BlockSpec(memory_space=pltpu.SMEM)
    vmem = pl.BlockSpec(memory_space=pltpu.VMEM)
    anywhere = pl.BlockSpec(memory_space=pl.ANY)
    column_parent, column_child, keep, give = pl.pallas_call(
        products_kernel,
        out_shape=(
            jax.ShapeDtypeStruct((blocks, pieces, strip, width), BF16),
            jax.ShapeDtypeStruct((blocks, pieces, strip, width), BF16),
            jax.ShapeDtypeStruct((procs // CORES, 3, pieces, strip, width), BF16),
            jax.ShapeDtypeStruct((procs // CORES, 3, pieces, strip, width), BF16),
        ),
        in_specs=[smem, vmem] + [anywhere] * 4 + [vmem] * 3,
        out_specs=(vmem, vmem, vmem, vmem),
        scratch_shapes=[
            pltpu.VMEM((YS, XS, CORES) + panels_shape[1:], BF16),
            pltpu.SemaphoreType.DMA((2, blocks, 4)),
        ],
        compiler_params=pltpu.CompilerParams(vmem_limit_bytes=32 * 1024 * 1024),
        interpret=INTERPRET,
        name="products",
    )(scalars, upper, *gathered_panels, panel_parent[0], panel_child[0], pivot_parent[0])
    sums = (keep.astype(F32) + moved(give, (0, 0, 1)).astype(F32)).astype(BF16)
    same_core = [[place * CORES + c for place in range(procs // CORES)] for c in range(CORES)]
    arrived = lax.all_to_all(
        sums, "proc", split_axis=0, concat_axis=0, tiled=True, axis_index_groups=same_core
    )
    whole = pl.BlockSpec((pieces, strip, width), lambda i: (0, 0, 0))
    block_parent, column_child, block_child = pl.pallas_call(
        final_kernel,
        grid=(1,),
        out_shape=(
            jax.ShapeDtypeStruct((pieces, strip, width), BF16),
            jax.ShapeDtypeStruct((blocks, pieces, strip, width), BF16),
            jax.ShapeDtypeStruct((pieces, strip, width), BF16),
        ),
        in_specs=[
            pl.BlockSpec(arrived.shape, lambda i: (0, 0, 0, 0, 0)),
            whole,
            whole,
            pl.BlockSpec(memory_space=pl.ANY),
        ],
        out_specs=(whole, pl.BlockSpec((1, pieces, strip, width), lambda i: (0, 0, 0, 0)), whole),
        input_output_aliases={3: 1},
        interpret=INTERPRET,
        name="final",
    )(arrived, pivot_parent[0], pivot_child[0], column_child)
    return column_parent[None], block_parent[None], column_child[None], block_child[None]


def solution(mesh):
    in_specs = (
        P("group", "proc", None),
        P(),
        P(),
        P(),
        P("group", None, None, "proc", None),
        P("group", None, None, "proc", None),
        P("group", None, "proc", None),
        P("group", None, "proc", None),
    )
    out_specs = (
        P("group", None, None, "proc", None),
        P("group", None, "proc", None),
        P("group", None, None, "proc", None),
        P("group", None, "proc", None),
    )

    return jax.shard_map(per_device, mesh=mesh, in_specs=in_specs, out_specs=out_specs, check_vma=False)
```

```python
import jax
import jax.numpy as jnp
from jax import lax
from jax.experimental import pallas as pl
from jax.experimental.pallas import tpu as pltpu
from jax.sharding import PartitionSpec as P


INTERPRET = False
YS, XS, CORES = 2, 4, 2
PROCS = YS * XS * CORES
F32 = jnp.float32
BF16 = jnp.bfloat16


def dot(a, b):
    return jnp.dot(a, b, preferred_element_type=F32)


def dot_rows(a, b):
    return lax.dot_general(a, b, (((0,), (0,)), ((), ())), preferred_element_type=F32)


def products_kernel(
    kept, upper, near, near_other, far, far_other, own_first, own_second, pivot, column_out, child_out, keep_out, give_out, panels, sems
):
    strip, pieces, blocks, slabs, half = upper.shape
    procs, width = PROCS, panels.shape[-1]
    rows = strip * slabs
    core, y = kept[blocks - 1], kept[blocks]
    sources = ((near, y, core), (near_other, y, 1 - core), (far, 1 - y, core), (far_other, 1 - y, 1 - core))
    many = blocks // 2
    copies = {}
    for n in range(2):
        for part in range(2):
            span = pl.ds(part * many, many)
            copies[n, part] = [
                pltpu.make_async_copy(source.at[:, n, span], panels.at[at_y, :, at_core, n, span], sems.at[n, part, k])
                for k, (source, at_y, at_core) in enumerate(sources)
            ]
            for copy in copies[n, part]:
                copy.start()

    def left(h, b):
        return upper[:, h, b].reshape(rows, half)

    def right(n, b, h):
        return panels[:, :, :, n, b, h].reshape(half, width)

    def arrive(n, b):
        if b % many == 0:
            for copy in copies[n, b // many]:
                copy.wait()

    total = jnp.zeros((rows, width), F32)
    for b in range(blocks):
        arrive(0, b)
        for h in range(pieces):
            total += dot(left(h, b), right(0, b, h))
    column = (-total).astype(BF16)
    at = lax.broadcasted_iota(jnp.int32, (rows, rows), 0)
    of = lax.broadcasted_iota(jnp.int32, (rows, rows), 1)
    same_row = (at % strip == of // slabs) & ((at // strip) % pieces == of % pieces)
    to_block = at // (strip * pieces)
    of_block = (of % slabs) // pieces
    wanted = jnp.full((rows, rows), -1, jnp.int32)
    for b in range(1, blocks):
        wanted = jnp.where(to_block == b, kept[b - 1], wanted)
    in_order = (same_row & (to_block == of_block)).astype(F32).astype(BF16)
    in_child = (same_row & (wanted == of_block)).astype(F32).astype(BF16)
    column_natural = dot(in_order, column).astype(BF16)
    column_kept = dot(in_child, column).astype(BF16)
    column_out[...] = column_natural.reshape(column_out.shape)

    arrive(1, 0)
    top = [right(1, 0, h) for h in range(pieces)]
    first = own_first[...].reshape(rows, width)
    second = own_second[...].reshape(rows, width)
    diagonal = pivot[...].reshape(strip * pieces, width)
    parent_sum = dot_rows(first, column_natural)
    cross = jnp.zeros((rows, width), F32)
    for h in range(pieces):
        cross += dot(first[:, h * half : (h + 1) * half], top[h])
    head_sum = (
        dot_rows(column_kept, second)
        - dot_rows(column_natural, cross.astype(BF16))
        + dot_rows(diagonal, second[: strip * pieces])
    ).astype(BF16)
    child_sum = jnp.zeros((width, width), F32)
    for h in range(pieces):
        child_sum += dot_rows(top[h], head_sum[h * half : (h + 1) * half])

    total = jnp.zeros((rows, width), F32)
    for b in range(1, blocks):
        arrive(1, b)
        for h in range(pieces):
            total += dot(left(h, kept[b - 1]), right(1, b, h))
    for h in range(pieces):
        total += dot(column[:, h * half : (h + 1) * half], top[h])
    child = dot(in_child, (-total).astype(BF16)).astype(BF16)
    child_out[...] = child.reshape(child_out.shape)
    child_sum -= dot_rows(second, child)
    for n, value in enumerate((parent_sum.astype(BF16), head_sum, child_sum.astype(BF16))):
        for h in range(pieces):
            for place in range(procs // CORES):
                start = h * half + place * CORES * strip
                a, b = value[start : start + strip], value[start + strip : start + CORES * strip]
                keep_out[place, n, h] = jnp.where(core == 0, a, b)
                give_out[place, n, h] = jnp.where(core == 0, b, a)


def final_kernel(arrived, pivot_first, pivot_second, child_in, block_first, child_out, block_second):
    del child_in
    sums = [arrived[0, n].astype(F32) for n in range(3)]
    for p in range(1, arrived.shape[0]):
        for n in range(3):
            sums[n] += arrived[p, n].astype(F32)
    block_first[...] = (pivot_first[...].astype(F32) - sums[0]).astype(BF16)
    child_out[0] = (-sums[1]).astype(BF16)
    block_second[...] = (pivot_second[...].astype(F32) + sums[2]).astype(BF16)


def moved(value, step):
    pairs = []
    for p in range(PROCS):
        y, x, core = p // (XS * CORES), p // CORES % XS, p % CORES
        y, x, core = (y + step[0]) % YS, (x + step[1]) % XS, (core + step[2]) % CORES
        pairs.append((p, (y * XS + x) * CORES + core))
    return lax.ppermute(value, "proc", pairs)


def assemble_kernel(place, *refs):
    out = refs[XS]
    for dx in range(XS):
        out[(place[0] - dx) & (XS - 1)] = refs[dx][...]


def shifted(shard):
    other = moved(shard, (1, 0, 0))
    rows = []
    for part in (shard, other):
        row = [part]
        for dx in range(1, XS):
            row.append(moved(part, (0, dx, 0)))
        rows.append(row)
    return rows


def gathered(rows):
    place = ((lax.axis_index("proc") >> 1) & (XS - 1))[None].astype(jnp.int32)
    vmem = pl.BlockSpec(memory_space=pltpu.VMEM)
    both = []
    for row in rows:
        together = pl.pallas_call(
            assemble_kernel,
            out_shape=jax.ShapeDtypeStruct((XS,) + row[0].shape, BF16),
            in_specs=[pl.BlockSpec(memory_space=pltpu.SMEM)] + [vmem] * XS,
            out_specs=vmem,
            compiler_params=pltpu.CompilerParams(vmem_limit_bytes=16 * 1024 * 1024),
            interpret=INTERPRET,
            name="assemble",
        )(place, *row)
        pair = [together, moved(together, (0, 0, 1))]
        both += [pltpu.with_memory_space_constraint(half, pltpu.HBM) for half in pair]
    return both


def per_device(
    ancestor_rows,
    piece_owner,
    structure,
    kept_blocks,
    panel_parent,
    panel_child,
    pivot_parent,
    pivot_child,
):
    group_index = lax.axis_index("group")
    strip = ancestor_rows.shape[1]
    groups, blocks = structure.shape
    procs = lax.axis_size("proc")
    pieces = panel_parent.shape[2]
    width = panel_parent.shape[-1]
    half = width // pieces
    tops = ancestor_rows.shape[2] // width
    slabs = blocks * pieces

    rows = shifted(jnp.stack([panel_parent[0], panel_child[0]]))

    spread = ancestor_rows.reshape(strip, tops, pieces, half).transpose(0, 2, 1, 3)
    spread = lax.all_to_all(
        spread.reshape(groups, tops, half), "group", split_axis=0, concat_axis=0, tiled=True
    )
    owners = piece_owner.reshape(tops, pieces)
    same = structure[:, :, None, None] == jnp.arange(tops, dtype=jnp.int32)[:, None]
    owner = jnp.where(same, owners, 0).sum(axis=2).reshape(groups, slabs)
    index = owner[:, None, :] * tops + structure[:, :, None]
    choice = jax.nn.one_hot(index.reshape(-1), groups * tops, dtype=BF16)
    outgoing = jnp.dot(choice, spread.reshape(groups * tops, half), preferred_element_type=BF16)
    panels_shape = (XS, 2) + panel_parent.shape[1:]
    gathered_panels = gathered(rows)
    upper = lax.all_to_all(
        outgoing.reshape(groups, blocks, slabs, half), "group", split_axis=0, concat_axis=0, tiled=True
    )
    upper = upper.reshape(strip, pieces, blocks, slabs, half)

    here = lax.axis_index("proc")
    place = jnp.stack([here & (CORES - 1), here >> 3]).astype(jnp.int32)
    scalars = jnp.concatenate([kept_blocks[group_index], place])
    smem = pl.BlockSpec(memory_space=pltpu.SMEM)
    vmem = pl.BlockSpec(memory_space=pltpu.VMEM)
    anywhere = pl.BlockSpec(memory_space=pl.ANY)
    column_parent, column_child, keep, give = pl.pallas_call(
        products_kernel,
        out_shape=(
            jax.ShapeDtypeStruct((blocks, pieces, strip, width), BF16),
            jax.ShapeDtypeStruct((blocks, pieces, strip, width), BF16),
            jax.ShapeDtypeStruct((procs // CORES, 3, pieces, strip, width), BF16),
            jax.ShapeDtypeStruct((procs // CORES, 3, pieces, strip, width), BF16),
        ),
        in_specs=[smem, vmem] + [anywhere] * 4 + [vmem] * 3,
        out_specs=(vmem, vmem, vmem, vmem),
        scratch_shapes=[
            pltpu.VMEM((YS, XS, CORES) + panels_shape[1:], BF16),
            pltpu.SemaphoreType.DMA((2, 2, 4)),
        ],
        compiler_params=pltpu.CompilerParams(vmem_limit_bytes=32 * 1024 * 1024),
        interpret=INTERPRET,
        name="products",
    )(scalars, upper, *gathered_panels, panel_parent[0], panel_child[0], pivot_parent[0])
    sums = (keep.astype(F32) + moved(give, (0, 0, 1)).astype(F32)).astype(BF16)
    same_core = [[place * CORES + c for place in range(procs // CORES)] for c in range(CORES)]
    arrived = lax.all_to_all(
        sums, "proc", split_axis=0, concat_axis=0, tiled=True, axis_index_groups=same_core
    )
    whole = pl.BlockSpec((pieces, strip, width), lambda i: (0, 0, 0))
    block_parent, column_child, block_child = pl.pallas_call(
        final_kernel,
        grid=(1,),
        out_shape=(
            jax.ShapeDtypeStruct((pieces, strip, width), BF16),
            jax.ShapeDtypeStruct((blocks, pieces, strip, width), BF16),
            jax.ShapeDtypeStruct((pieces, strip, width), BF16),
        ),
        in_specs=[
            pl.BlockSpec(arrived.shape, lambda i: (0, 0, 0, 0, 0)),
            whole,
            whole,
            pl.BlockSpec(memory_space=pl.ANY),
        ],
        out_specs=(whole, pl.BlockSpec((1, pieces, strip, width), lambda i: (0, 0, 0, 0)), whole),
        input_output_aliases={3: 1},
        interpret=INTERPRET,
        name="final",
    )(arrived, pivot_parent[0], pivot_child[0], column_child)
    return column_parent[None], block_parent[None], column_child[None], block_child[None]


def solution(mesh):
    in_specs = (
        P("group", "proc", None),
        P(),
        P(),
        P(),
        P("group", None, None, "proc", None),
        P("group", None, None, "proc", None),
        P("group", None, "proc", None),
        P("group", None, "proc", None),
    )
    out_specs = (
        P("group", None, None, "proc", None),
        P("group", None, "proc", None),
        P("group", None, None, "proc", None),
        P("group", None, "proc", None),
    )

    return jax.shard_map(per_device, mesh=mesh, in_specs=in_specs, out_specs=out_specs, check_vma=False)
```

```python
import jax
import jax.numpy as jnp
from jax import lax
from jax.experimental import pallas as pl
from jax.experimental.pallas import tpu as pltpu
from jax.sharding import PartitionSpec as P


INTERPRET = False
YS, XS, CORES = 2, 4, 2
PROCS = YS * XS * CORES
F32 = jnp.float32
BF16 = jnp.bfloat16


def dot(a, b):
    return jnp.dot(a, b, preferred_element_type=F32)


def dot_rows(a, b):
    return lax.dot_general(a, b, (((0,), (0,)), ((), ())), preferred_element_type=F32)


def products_kernel(
    kept, upper, near, near_other, far, far_other, own_first, own_second, pivot, column_out, child_out, keep_out, give_out, panels, sems
):
    strip, pieces, blocks, slabs, half = upper.shape
    procs, width = PROCS, panels.shape[-1]
    rows = strip * slabs
    core, y = kept[blocks - 1], kept[blocks]
    sources = ((near, y, core), (near_other, y, 1 - core), (far, 1 - y, core), (far_other, 1 - y, 1 - core))
    many = blocks // 2
    copies = {}
    for n in range(2):
        for part in range(2):
            span = pl.ds(part * many, many)
            copies[n, part] = [
                pltpu.make_async_copy(source.at[:, n, span], panels.at[at_y, :, at_core, n, span], sems.at[n, part, k])
                for k, (source, at_y, at_core) in enumerate(sources)
            ]
            for copy in copies[n, part]:
                copy.start()

    def left(h, b):
        return upper[:, h, b].reshape(rows, half)

    def right(n, b, h):
        return panels[:, :, :, n, b, h].reshape(half, width)

    def arrive(n, b):
        if b % many == 0:
            for copy in copies[n, b // many]:
                copy.wait()

    total = jnp.zeros((rows, width), F32)
    for b in range(blocks):
        arrive(0, b)
        for h in range(pieces):
            total += dot(left(h, b), right(0, b, h))
    column = (-total).astype(BF16)
    at = lax.broadcasted_iota(jnp.int32, (rows, rows), 0)
    of = lax.broadcasted_iota(jnp.int32, (rows, rows), 1)
    same_row = (at % strip == of // slabs) & ((at // strip) % pieces == of % pieces)
    to_block = at // (strip * pieces)
    of_block = (of % slabs) // pieces
    wanted = jnp.full((rows, rows), -1, jnp.int32)
    for b in range(1, blocks):
        wanted = jnp.where(to_block == b, kept[b - 1], wanted)
    in_order = (same_row & (to_block == of_block)).astype(F32).astype(BF16)
    in_child = (same_row & (wanted == of_block)).astype(F32).astype(BF16)
    column_natural = dot(in_order, column).astype(BF16)
    column_kept = dot(in_child, column).astype(BF16)
    column_out[...] = column_natural.reshape(column_out.shape)

    arrive(1, 0)
    top = [right(1, 0, h) for h in range(pieces)]
    first = own_first[...].reshape(rows, width)
    second = own_second[...].reshape(rows, width)
    diagonal = pivot[...].reshape(strip * pieces, width)
    parent_sum = dot_rows(first, column_natural)
    cross = jnp.zeros((rows, width), F32)
    for h in range(pieces):
        cross += dot(first[:, h * half : (h + 1) * half], top[h])
    head_sum = (
        dot_rows(column_kept, second)
        - dot_rows(column_natural, cross.astype(BF16))
        + dot_rows(diagonal, second[: strip * pieces])
    ).astype(BF16)
    child_sum = jnp.zeros((width, width), F32)
    for h in range(pieces):
        child_sum += dot_rows(top[h], head_sum[h * half : (h + 1) * half])

    total = jnp.zeros((rows, width), F32)
    for b in range(1, blocks):
        arrive(1, b)
        for h in range(pieces):
            total += dot(left(h, kept[b - 1]), right(1, b, h))
    for h in range(pieces):
        total += dot(column[:, h * half : (h + 1) * half], top[h])
    child = dot(in_child, (-total).astype(BF16)).astype(BF16)
    child_out[...] = child.reshape(child_out.shape)
    child_sum -= dot_rows(second, child)
    for n, value in enumerate((parent_sum.astype(BF16), head_sum, child_sum.astype(BF16))):
        for h in range(pieces):
            for place in range(procs // CORES):
                start = h * half + place * CORES * strip
                a, b = value[start : start + strip], value[start + strip : start + CORES * strip]
                keep_out[place, n, h] = jnp.where(core == 0, a, b)
                give_out[place, n, h] = jnp.where(core == 0, b, a)


def final_kernel(arrived, pivot_first, pivot_second, child_in, block_first, child_out, block_second):
    del child_in
    sums = [arrived[0, n].astype(F32) for n in range(3)]
    for p in range(1, arrived.shape[0]):
        for n in range(3):
            sums[n] += arrived[p, n].astype(F32)
    block_first[...] = (pivot_first[...].astype(F32) - sums[0]).astype(BF16)
    child_out[0] = (-sums[1]).astype(BF16)
    block_second[...] = (pivot_second[...].astype(F32) + sums[2]).astype(BF16)


def moved(value, step):
    pairs = []
    for p in range(PROCS):
        y, x, core = p // (XS * CORES), p // CORES % XS, p % CORES
        y, x, core = (y + step[0]) % YS, (x + step[1]) % XS, (core + step[2]) % CORES
        pairs.append((p, (y * XS + x) * CORES + core))
    return lax.ppermute(value, "proc", pairs)


def assemble_kernel(place, *refs):
    out = refs[XS]
    for dx in range(XS):
        out[(place[0] - dx) & (XS - 1)] = refs[dx][...]


def shifted(shard):
    other = moved(shard, (1, 0, 0))
    back = moved(shard, (0, XS - 1, 0))
    other_on = moved(other, (0, 1, 0))
    back_twice = moved(back, (0, XS - 1, 0))
    on = moved(shard, (0, 1, 0))
    other_back = moved(other, (0, XS - 1, 0))
    other_on_twice = moved(other_on, (0, 1, 0))
    return (shard, on, back_twice, back), (other, other_on, other_on_twice, other_back)


def gathered(rows):
    place = ((lax.axis_index("proc") >> 1) & (XS - 1))[None].astype(jnp.int32)
    vmem = pl.BlockSpec(memory_space=pltpu.VMEM)
    both = []
    for row in rows:
        together = pl.pallas_call(
            assemble_kernel,
            out_shape=jax.ShapeDtypeStruct((XS,) + row[0].shape, BF16),
            in_specs=[pl.BlockSpec(memory_space=pltpu.SMEM)] + [vmem] * XS,
            out_specs=vmem,
            compiler_params=pltpu.CompilerParams(vmem_limit_bytes=16 * 1024 * 1024),
            interpret=INTERPRET,
            name="assemble",
        )(place, *row)
        pair = [together, moved(together, (0, 0, 1))]
        both += [pltpu.with_memory_space_constraint(half, pltpu.HBM) for half in pair]
    return both


def per_device(
    ancestor_rows,
    piece_owner,
    structure,
    kept_blocks,
    panel_parent,
    panel_child,
    pivot_parent,
    pivot_child,
):
    group_index = lax.axis_index("group")
    strip = ancestor_rows.shape[1]
    groups, blocks = structure.shape
    procs = lax.axis_size("proc")
    pieces = panel_parent.shape[2]
    width = panel_parent.shape[-1]
    half = width // pieces
    tops = ancestor_rows.shape[2] // width
    slabs = blocks * pieces

    rows = shifted(jnp.stack([panel_parent[0], panel_child[0]]))

    spread = ancestor_rows.reshape(strip, tops, pieces, half).transpose(0, 2, 1, 3)
    spread = lax.all_to_all(
        spread.reshape(groups, tops, half), "group", split_axis=0, concat_axis=0, tiled=True
    )
    owners = piece_owner.reshape(tops, pieces)
    same = structure[:, :, None, None] == jnp.arange(tops, dtype=jnp.int32)[:, None]
    owner = jnp.where(same, owners, 0).sum(axis=2).reshape(groups, slabs)
    index = owner[:, None, :] * tops + structure[:, :, None]
    choice = jax.nn.one_hot(index.reshape(-1), groups * tops, dtype=BF16)
    outgoing = jnp.dot(choice, spread.reshape(groups * tops, half), preferred_element_type=BF16)
    panels_shape = (XS, 2) + panel_parent.shape[1:]
    gathered_panels = gathered(rows)
    upper = lax.all_to_all(
        outgoing.reshape(groups, blocks, slabs, half), "group", split_axis=0, concat_axis=0, tiled=True
    )
    upper = upper.reshape(strip, pieces, blocks, slabs, half)

    here = lax.axis_index("proc")
    place = jnp.stack([here & (CORES - 1), here >> 3]).astype(jnp.int32)
    scalars = jnp.concatenate([kept_blocks[group_index], place])
    smem = pl.BlockSpec(memory_space=pltpu.SMEM)
    vmem = pl.BlockSpec(memory_space=pltpu.VMEM)
    anywhere = pl.BlockSpec(memory_space=pl.ANY)
    column_parent, column_child, keep, give = pl.pallas_call(
        products_kernel,
        out_shape=(
            jax.ShapeDtypeStruct((blocks, pieces, strip, width), BF16),
            jax.ShapeDtypeStruct((blocks, pieces, strip, width), BF16),
            jax.ShapeDtypeStruct((procs // CORES, 3, pieces, strip, width), BF16),
            jax.ShapeDtypeStruct((procs // CORES, 3, pieces, strip, width), BF16),
        ),
        in_specs=[smem, vmem] + [anywhere] * 4 + [vmem] * 3,
        out_specs=(vmem, vmem, vmem, vmem),
        scratch_shapes=[
            pltpu.VMEM((YS, XS, CORES) + panels_shape[1:], BF16),
            pltpu.SemaphoreType.DMA((2, 2, 4)),
        ],
        compiler_params=pltpu.CompilerParams(vmem_limit_bytes=32 * 1024 * 1024),
        interpret=INTERPRET,
        name="products",
    )(scalars, upper, *gathered_panels, panel_parent[0], panel_child[0], pivot_parent[0])
    sums = (keep.astype(F32) + moved(give, (0, 0, 1)).astype(F32)).astype(BF16)
    same_core = [[place * CORES + c for place in range(procs // CORES)] for c in range(CORES)]
    arrived = lax.all_to_all(
        sums, "proc", split_axis=0, concat_axis=0, tiled=True, axis_index_groups=same_core
    )
    whole = pl.BlockSpec((pieces, strip, width), lambda i: (0, 0, 0))
    block_parent, column_child, block_child = pl.pallas_call(
        final_kernel,
        grid=(1,),
        out_shape=(
            jax.ShapeDtypeStruct((pieces, strip, width), BF16),
            jax.ShapeDtypeStruct((blocks, pieces, strip, width), BF16),
            jax.ShapeDtypeStruct((pieces, strip, width), BF16),
        ),
        in_specs=[
            pl.BlockSpec(arrived.shape, lambda i: (0, 0, 0, 0, 0)),
            whole,
            whole,
            pl.BlockSpec(memory_space=pl.ANY),
        ],
        out_specs=(whole, pl.BlockSpec((1, pieces, strip, width), lambda i: (0, 0, 0, 0)), whole),
        input_output_aliases={3: 1},
        interpret=INTERPRET,
        name="final",
    )(arrived, pivot_parent[0], pivot_child[0], column_child)
    return column_parent[None], block_parent[None], column_child[None], block_child[None]


def solution(mesh):
    in_specs = (
        P("group", "proc", None),
        P(),
        P(),
        P(),
        P("group", None, None, "proc", None),
        P("group", None, None, "proc", None),
        P("group", None, "proc", None),
        P("group", None, "proc", None),
    )
    out_specs = (
        P("group", None, None, "proc", None),
        P("group", None, "proc", None),
        P("group", None, None, "proc", None),
        P("group", None, "proc", None),
    )

    return jax.shard_map(per_device, mesh=mesh, in_specs=in_specs, out_specs=out_specs, check_vma=False)
```

```python
import jax
import jax.numpy as jnp
from jax import lax
from jax.experimental import pallas as pl
from jax.experimental.pallas import tpu as pltpu
from jax.sharding import PartitionSpec as P


INTERPRET = False
YS, XS, CORES = 2, 4, 2
PROCS = YS * XS * CORES
F32 = jnp.float32
BF16 = jnp.bfloat16


def dot(a, b):
    return jnp.dot(a, b, preferred_element_type=F32)


def dot_rows(a, b):
    return lax.dot_general(a, b, (((0,), (0,)), ((), ())), preferred_element_type=F32)


def products_kernel(
    kept, upper, near, near_other, far, far_other, own_first, own_second, pivot, column_out, child_out, keep_out, give_out, panels, sems
):
    strip, pieces, blocks, slabs, half = upper.shape
    procs, width = PROCS, panels.shape[-1]
    rows = strip * slabs
    core, y = kept[blocks - 1], kept[blocks]
    sources = ((near, y, core), (near_other, y, 1 - core), (far, 1 - y, core), (far_other, 1 - y, 1 - core))
    many = blocks // 2
    copies = {}
    for n in range(2):
        for part in range(2):
            span = pl.ds(part * many, many)
            copies[n, part] = [
                pltpu.make_async_copy(source.at[:, n, span], panels.at[at_y, :, at_core, n, span], sems.at[n, part, k])
                for k, (source, at_y, at_core) in enumerate(sources)
            ]
            for copy in copies[n, part]:
                copy.start()

    def left(h, b):
        return upper[:, h, b].reshape(rows, half)

    def right(n, b, h):
        return panels[:, :, :, n, b, h].reshape(half, width)

    def wide(b):
        return jnp.concatenate([left(h, b) for h in range(pieces)], axis=1)

    def tall(n, b):
        return jnp.concatenate([right(n, b, h) for h in range(pieces)], axis=0)

    def arrive(n, b):
        if b % many == 0:
            for copy in copies[n, b // many]:
                copy.wait()

    total = jnp.zeros((rows, width), F32)
    for b in range(blocks):
        arrive(0, b)
        total += dot(wide(b), tall(0, b))
    column = (-total).astype(BF16)
    at = lax.broadcasted_iota(jnp.int32, (rows, rows), 0)
    of = lax.broadcasted_iota(jnp.int32, (rows, rows), 1)
    same_row = (at % strip == of // slabs) & ((at // strip) % pieces == of % pieces)
    to_block = at // (strip * pieces)
    of_block = (of % slabs) // pieces
    wanted = jnp.full((rows, rows), -1, jnp.int32)
    for b in range(1, blocks):
        wanted = jnp.where(to_block == b, kept[b - 1], wanted)
    in_order = (same_row & (to_block == of_block)).astype(F32).astype(BF16)
    in_child = (same_row & (wanted == of_block)).astype(F32).astype(BF16)
    column_natural = dot(in_order, column).astype(BF16)
    column_kept = dot(in_child, column).astype(BF16)
    column_out[...] = column_natural.reshape(column_out.shape)

    arrive(1, 0)
    top = tall(1, 0)
    first = own_first[...].reshape(rows, width)
    second = own_second[...].reshape(rows, width)
    diagonal = pivot[...].reshape(strip * pieces, width)
    parent_sum = dot_rows(first, column_natural)
    cross = dot(first, top)
    head_sum = (
        dot_rows(column_kept, second)
        - dot_rows(column_natural, cross.astype(BF16))
        + dot_rows(diagonal, second[: strip * pieces])
    ).astype(BF16)
    child_sum = dot_rows(top, head_sum)

    total = jnp.zeros((rows, width), F32)
    for b in range(1, blocks):
        arrive(1, b)
        total += dot(wide(kept[b - 1]), tall(1, b))
    total += dot(column, top)
    child = dot(in_child, (-total).astype(BF16)).astype(BF16)
    child_out[...] = child.reshape(child_out.shape)
    child_sum -= dot_rows(second, child)
    for n, value in enumerate((parent_sum.astype(BF16), head_sum, child_sum.astype(BF16))):
        for h in range(pieces):
            for place in range(procs // CORES):
                start = h * half + place * CORES * strip
                a, b = value[start : start + strip], value[start + strip : start + CORES * strip]
                keep_out[place, n, h] = jnp.where(core == 0, a, b)
                give_out[place, n, h] = jnp.where(core == 0, b, a)


def final_kernel(arrived, pivot_first, pivot_second, child_in, block_first, child_out, block_second):
    del child_in
    sums = [arrived[0, n].astype(F32) for n in range(3)]
    for p in range(1, arrived.shape[0]):
        for n in range(3):
            sums[n] += arrived[p, n].astype(F32)
    block_first[...] = (pivot_first[...].astype(F32) - sums[0]).astype(BF16)
    child_out[0] = (-sums[1]).astype(BF16)
    block_second[...] = (pivot_second[...].astype(F32) + sums[2]).astype(BF16)


def moved(value, step):
    pairs = []
    for p in range(PROCS):
        y, x, core = p // (XS * CORES), p // CORES % XS, p % CORES
        y, x, core = (y + step[0]) % YS, (x + step[1]) % XS, (core + step[2]) % CORES
        pairs.append((p, (y * XS + x) * CORES + core))
    return lax.ppermute(value, "proc", pairs)


def assemble_kernel(place, *refs):
    out = refs[XS]
    for dx in range(XS):
        out[(place[0] - dx) & (XS - 1)] = refs[dx][...]


def shifted(shard):
    other = moved(shard, (1, 0, 0))
    back = moved(shard, (0, XS - 1, 0))
    other_on = moved(other, (0, 1, 0))
    back_twice = moved(back, (0, XS - 1, 0))
    on = moved(shard, (0, 1, 0))
    other_back = moved(other, (0, XS - 1, 0))
    other_on_twice = moved(other_on, (0, 1, 0))
    return (shard, on, back_twice, back), (other, other_on, other_on_twice, other_back)


def gathered(rows):
    place = ((lax.axis_index("proc") >> 1) & (XS - 1))[None].astype(jnp.int32)
    vmem = pl.BlockSpec(memory_space=pltpu.VMEM)
    both = []
    for row in rows:
        together = pl.pallas_call(
            assemble_kernel,
            out_shape=jax.ShapeDtypeStruct((XS,) + row[0].shape, BF16),
            in_specs=[pl.BlockSpec(memory_space=pltpu.SMEM)] + [vmem] * XS,
            out_specs=vmem,
            compiler_params=pltpu.CompilerParams(vmem_limit_bytes=16 * 1024 * 1024),
            interpret=INTERPRET,
            name="assemble",
        )(place, *row)
        pair = [together, moved(together, (0, 0, 1))]
        both += [pltpu.with_memory_space_constraint(half, pltpu.HBM) for half in pair]
    return both


def per_device(
    ancestor_rows,
    piece_owner,
    structure,
    kept_blocks,
    panel_parent,
    panel_child,
    pivot_parent,
    pivot_child,
):
    group_index = lax.axis_index("group")
    strip = ancestor_rows.shape[1]
    groups, blocks = structure.shape
    procs = lax.axis_size("proc")
    pieces = panel_parent.shape[2]
    width = panel_parent.shape[-1]
    half = width // pieces
    tops = ancestor_rows.shape[2] // width
    slabs = blocks * pieces

    rows = shifted(jnp.stack([panel_parent[0], panel_child[0]]))

    spread = ancestor_rows.reshape(strip, tops, pieces, half).transpose(0, 2, 1, 3)
    spread = lax.all_to_all(
        spread.reshape(groups, tops, half), "group", split_axis=0, concat_axis=0, tiled=True
    )
    owners = piece_owner.reshape(tops, pieces)
    same = structure[:, :, None, None] == jnp.arange(tops, dtype=jnp.int32)[:, None]
    owner = jnp.where(same, owners, 0).sum(axis=2).reshape(groups, slabs)
    index = owner[:, None, :] * tops + structure[:, :, None]
    choice = jax.nn.one_hot(index.reshape(-1), groups * tops, dtype=BF16)
    outgoing = jnp.dot(choice, spread.reshape(groups * tops, half), preferred_element_type=BF16)
    panels_shape = (XS, 2) + panel_parent.shape[1:]
    gathered_panels = gathered(rows)
    upper = lax.all_to_all(
        outgoing.reshape(groups, blocks, slabs, half), "group", split_axis=0, concat_axis=0, tiled=True
    )
    upper = upper.reshape(strip, pieces, blocks, slabs, half)

    here = lax.axis_index("proc")
    place = jnp.stack([here & (CORES - 1), here >> 3]).astype(jnp.int32)
    scalars = jnp.concatenate([kept_blocks[group_index], place])
    smem = pl.BlockSpec(memory_space=pltpu.SMEM)
    vmem = pl.BlockSpec(memory_space=pltpu.VMEM)
    anywhere = pl.BlockSpec(memory_space=pl.ANY)
    column_parent, column_child, keep, give = pl.pallas_call(
        products_kernel,
        out_shape=(
            jax.ShapeDtypeStruct((blocks, pieces, strip, width), BF16),
            jax.ShapeDtypeStruct((blocks, pieces, strip, width), BF16),
            jax.ShapeDtypeStruct((procs // CORES, 3, pieces, strip, width), BF16),
            jax.ShapeDtypeStruct((procs // CORES, 3, pieces, strip, width), BF16),
        ),
        in_specs=[smem, vmem] + [anywhere] * 4 + [vmem] * 3,
        out_specs=(vmem, vmem, vmem, vmem),
        scratch_shapes=[
            pltpu.VMEM((YS, XS, CORES) + panels_shape[1:], BF16),
            pltpu.SemaphoreType.DMA((2, 2, 4)),
        ],
        compiler_params=pltpu.CompilerParams(vmem_limit_bytes=32 * 1024 * 1024),
        interpret=INTERPRET,
        name="products",
    )(scalars, upper, *gathered_panels, panel_parent[0], panel_child[0], pivot_parent[0])
    sums = (keep.astype(F32) + moved(give, (0, 0, 1)).astype(F32)).astype(BF16)
    same_core = [[place * CORES + c for place in range(procs // CORES)] for c in range(CORES)]
    arrived = lax.all_to_all(
        sums, "proc", split_axis=0, concat_axis=0, tiled=True, axis_index_groups=same_core
    )
    whole = pl.BlockSpec((pieces, strip, width), lambda i: (0, 0, 0))
    block_parent, column_child, block_child = pl.pallas_call(
        final_kernel,
        grid=(1,),
        out_shape=(
            jax.ShapeDtypeStruct((pieces, strip, width), BF16),
            jax.ShapeDtypeStruct((blocks, pieces, strip, width), BF16),
            jax.ShapeDtypeStruct((pieces, strip, width), BF16),
        ),
        in_specs=[
            vmem,
            whole,
            whole,
            pl.BlockSpec(memory_space=pl.ANY),
        ],
        out_specs=(whole, pl.BlockSpec((1, pieces, strip, width), lambda i: (0, 0, 0, 0)), whole),
        input_output_aliases={3: 1},
        compiler_params=pltpu.CompilerParams(vmem_limit_bytes=8 * 1024 * 1024),
        interpret=INTERPRET,
        name="final",
    )(arrived, pivot_parent[0], pivot_child[0], column_child)
    return column_parent[None], block_parent[None], column_child[None], block_child[None]


def solution(mesh):
    in_specs = (
        P("group", "proc", None),
        P(),
        P(),
        P(),
        P("group", None, None, "proc", None),
        P("group", None, None, "proc", None),
        P("group", None, "proc", None),
        P("group", None, "proc", None),
    )
    out_specs = (
        P("group", None, None, "proc", None),
        P("group", None, "proc", None),
        P("group", None, None, "proc", None),
        P("group", None, "proc", None),
    )

    return jax.shard_map(per_device, mesh=mesh, in_specs=in_specs, out_specs=out_specs, check_vma=False)
```

```python
import jax
import jax.numpy as jnp
from jax import lax
from jax.experimental import pallas as pl
from jax.experimental.pallas import tpu as pltpu
from jax.sharding import PartitionSpec as P


INTERPRET = False
YS, XS, CORES = 2, 4, 2
PROCS = YS * XS * CORES
F32 = jnp.float32
BF16 = jnp.bfloat16


def dot(a, b):
    return jnp.dot(a, b, preferred_element_type=F32)


def dot_rows(a, b):
    return lax.dot_general(a, b, (((0,), (0,)), ((), ())), preferred_element_type=F32)


def products_kernel(
    kept, upper, near, near_other, far, far_other, own_first, own_second, pivot, column_out, child_out, keep_out, give_out, panels, sems
):
    strip, pieces, blocks, slabs, half = upper.shape
    procs, width = PROCS, panels.shape[-1]
    rows = strip * slabs
    core, y = kept[blocks - 1], kept[blocks]
    sources = ((near, y, core), (near_other, y, 1 - core), (far, 1 - y, core), (far_other, 1 - y, 1 - core))
    starts = ((0, blocks // 2), (0, blocks - 2))
    copies = {}
    for n in range(2):
        for part in range(2):
            ends = starts[n][1:] + (blocks,)
            span = pl.ds(starts[n][part], ends[part] - starts[n][part])
            copies[n, part] = [
                pltpu.make_async_copy(source.at[:, n, span], panels.at[at_y, :, at_core, n, span], sems.at[n, part, k])
                for k, (source, at_y, at_core) in enumerate(sources)
            ]
            for copy in copies[n, part]:
                copy.start()

    def left(h, b):
        return upper[:, h, b].reshape(rows, half)

    def right(n, b, h):
        return panels[:, :, :, n, b, h].reshape(half, width)

    def wide(b):
        return jnp.concatenate([left(h, b) for h in range(pieces)], axis=1)

    def tall(n, b):
        return jnp.concatenate([right(n, b, h) for h in range(pieces)], axis=0)

    def arrive(n, b):
        if b in starts[n]:
            for copy in copies[n, starts[n].index(b)]:
                copy.wait()

    total = jnp.zeros((rows, width), F32)
    for b in range(blocks):
        arrive(0, b)
        total += dot(wide(b), tall(0, b))
    column = (-total).astype(BF16)
    at = lax.broadcasted_iota(jnp.int32, (rows, rows), 0)
    of = lax.broadcasted_iota(jnp.int32, (rows, rows), 1)
    same_row = (at % strip == of // slabs) & ((at // strip) % pieces == of % pieces)
    to_block = at // (strip * pieces)
    of_block = (of % slabs) // pieces
    wanted = jnp.full((rows, rows), -1, jnp.int32)
    for b in range(1, blocks):
        wanted = jnp.where(to_block == b, kept[b - 1], wanted)
    in_order = (same_row & (to_block == of_block)).astype(F32).astype(BF16)
    in_child = (same_row & (wanted == of_block)).astype(F32).astype(BF16)
    column_natural = dot(in_order, column).astype(BF16)
    column_kept = dot(in_child, column).astype(BF16)
    column_out[...] = column_natural.reshape(column_out.shape)

    arrive(1, 0)
    top = tall(1, 0)
    first = own_first[...].reshape(rows, width)
    second = own_second[...].reshape(rows, width)
    diagonal = pivot[...].reshape(strip * pieces, width)
    parent_sum = dot_rows(first, column_natural)
    cross = dot(first, top)
    head_sum = (
        dot_rows(column_kept, second)
        - dot_rows(column_natural, cross.astype(BF16))
        + dot_rows(diagonal, second[: strip * pieces])
    ).astype(BF16)
    child_sum = dot_rows(top, head_sum)

    total = jnp.zeros((rows, width), F32)
    for b in range(1, blocks):
        arrive(1, b)
        total += dot(wide(kept[b - 1]), tall(1, b))
    total += dot(column, top)
    child = dot(in_child, (-total).astype(BF16)).astype(BF16)
    child_out[...] = child.reshape(child_out.shape)
    child_sum -= dot_rows(second, child)
    for n, value in enumerate((parent_sum.astype(BF16), head_sum, child_sum.astype(BF16))):
        for h in range(pieces):
            for place in range(procs // CORES):
                start = h * half + place * CORES * strip
                a, b = value[start : start + strip], value[start + strip : start + CORES * strip]
                keep_out[place, n, h] = jnp.where(core == 0, a, b)
                give_out[place, n, h] = jnp.where(core == 0, b, a)


def final_kernel(arrived, pivot_first, pivot_second, child_in, block_first, child_out, block_second):
    del child_in
    sums = [arrived[0, n].astype(F32) for n in range(3)]
    for p in range(1, arrived.shape[0]):
        for n in range(3):
            sums[n] += arrived[p, n].astype(F32)
    block_first[...] = (pivot_first[...].astype(F32) - sums[0]).astype(BF16)
    child_out[0] = (-sums[1]).astype(BF16)
    block_second[...] = (pivot_second[...].astype(F32) + sums[2]).astype(BF16)


def moved(value, step):
    pairs = []
    for p in range(PROCS):
        y, x, core = p // (XS * CORES), p // CORES % XS, p % CORES
        y, x, core = (y + step[0]) % YS, (x + step[1]) % XS, (core + step[2]) % CORES
        pairs.append((p, (y * XS + x) * CORES + core))
    return lax.ppermute(value, "proc", pairs)


def assemble_kernel(place, *refs):
    out = refs[XS]
    for dx in range(XS):
        out[(place[0] - dx) & (XS - 1)] = refs[dx][...]


def shifted(shard):
    other = moved(shard, (1, 0, 0))
    back = moved(shard, (0, XS - 1, 0))
    other_on = moved(other, (0, 1, 0))
    back_twice = moved(back, (0, XS - 1, 0))
    on = moved(shard, (0, 1, 0))
    other_back = moved(other, (0, XS - 1, 0))
    other_on_twice = moved(other_on, (0, 1, 0))
    return (shard, on, back_twice, back), (other, other_on, other_on_twice, other_back)


def gathered(rows):
    place = ((lax.axis_index("proc") >> 1) & (XS - 1))[None].astype(jnp.int32)
    vmem = pl.BlockSpec(memory_space=pltpu.VMEM)
    both = []
    for row in rows:
        together = pl.pallas_call(
            assemble_kernel,
            out_shape=jax.ShapeDtypeStruct((XS,) + row[0].shape, BF16),
            in_specs=[pl.BlockSpec(memory_space=pltpu.SMEM)] + [vmem] * XS,
            out_specs=vmem,
            compiler_params=pltpu.CompilerParams(vmem_limit_bytes=16 * 1024 * 1024),
            interpret=INTERPRET,
            name="assemble",
        )(place, *row)
        pair = [together, moved(together, (0, 0, 1))]
        both += [pltpu.with_memory_space_constraint(half, pltpu.HBM) for half in pair]
    return both


def per_device(
    ancestor_rows,
    piece_owner,
    structure,
    kept_blocks,
    panel_parent,
    panel_child,
    pivot_parent,
    pivot_child,
):
    group_index = lax.axis_index("group")
    strip = ancestor_rows.shape[1]
    groups, blocks = structure.shape
    procs = lax.axis_size("proc")
    pieces = panel_parent.shape[2]
    width = panel_parent.shape[-1]
    half = width // pieces
    tops = ancestor_rows.shape[2] // width
    slabs = blocks * pieces

    rows = shifted(jnp.stack([panel_parent[0], panel_child[0]]))

    spread = ancestor_rows.reshape(strip, tops, pieces, half).transpose(0, 2, 1, 3)
    spread = lax.all_to_all(
        spread.reshape(groups, tops, half), "group", split_axis=0, concat_axis=0, tiled=True
    )
    owners = piece_owner.reshape(tops, pieces)
    same = structure[:, :, None, None] == jnp.arange(tops, dtype=jnp.int32)[:, None]
    owner = jnp.where(same, owners, 0).sum(axis=2).reshape(groups, slabs)
    index = owner[:, None, :] * tops + structure[:, :, None]
    choice = jax.nn.one_hot(index.reshape(-1), groups * tops, dtype=BF16)
    outgoing = jnp.dot(choice, spread.reshape(groups * tops, half), preferred_element_type=BF16)
    panels_shape = (XS, 2) + panel_parent.shape[1:]
    gathered_panels = gathered(rows)
    upper = lax.all_to_all(
        outgoing.reshape(groups, blocks, slabs, half), "group", split_axis=0, concat_axis=0, tiled=True
    )
    upper = upper.reshape(strip, pieces, blocks, slabs, half)

    here = lax.axis_index("proc")
    place = jnp.stack([here & (CORES - 1), here >> 3]).astype(jnp.int32)
    scalars = jnp.concatenate([kept_blocks[group_index], place])
    smem = pl.BlockSpec(memory_space=pltpu.SMEM)
    vmem = pl.BlockSpec(memory_space=pltpu.VMEM)
    anywhere = pl.BlockSpec(memory_space=pl.ANY)
    column_parent, column_child, keep, give = pl.pallas_call(
        products_kernel,
        out_shape=(
            jax.ShapeDtypeStruct((blocks, pieces, strip, width), BF16),
            jax.ShapeDtypeStruct((blocks, pieces, strip, width), BF16),
            jax.ShapeDtypeStruct((procs // CORES, 3, pieces, strip, width), BF16),
            jax.ShapeDtypeStruct((procs // CORES, 3, pieces, strip, width), BF16),
        ),
        in_specs=[smem, vmem] + [anywhere] * 4 + [vmem] * 3,
        out_specs=(vmem, vmem, vmem, vmem),
        scratch_shapes=[
            pltpu.VMEM((YS, XS, CORES) + panels_shape[1:], BF16),
            pltpu.SemaphoreType.DMA((2, 2, 4)),
        ],
        compiler_params=pltpu.CompilerParams(vmem_limit_bytes=32 * 1024 * 1024),
        interpret=INTERPRET,
        name="products",
    )(scalars, upper, *gathered_panels, panel_parent[0], panel_child[0], pivot_parent[0])
    sums = (keep.astype(F32) + moved(give, (0, 0, 1)).astype(F32)).astype(BF16)
    same_core = [[place * CORES + c for place in range(procs // CORES)] for c in range(CORES)]
    arrived = lax.all_to_all(
        sums, "proc", split_axis=0, concat_axis=0, tiled=True, axis_index_groups=same_core
    )
    whole = pl.BlockSpec((pieces, strip, width), lambda i: (0, 0, 0))
    block_parent, column_child, block_child = pl.pallas_call(
        final_kernel,
        grid=(1,),
        out_shape=(
            jax.ShapeDtypeStruct((pieces, strip, width), BF16),
            jax.ShapeDtypeStruct((blocks, pieces, strip, width), BF16),
            jax.ShapeDtypeStruct((pieces, strip, width), BF16),
        ),
        in_specs=[
            vmem,
            whole,
            whole,
            pl.BlockSpec(memory_space=pl.ANY),
        ],
        out_specs=(whole, pl.BlockSpec((1, pieces, strip, width), lambda i: (0, 0, 0, 0)), whole),
        input_output_aliases={3: 1},
        compiler_params=pltpu.CompilerParams(vmem_limit_bytes=8 * 1024 * 1024),
        interpret=INTERPRET,
        name="final",
    )(arrived, pivot_parent[0], pivot_child[0], column_child)
    return column_parent[None], block_parent[None], column_child[None], block_child[None]


def solution(mesh):
    in_specs = (
        P("group", "proc", None),
        P(),
        P(),
        P(),
        P("group", None, None, "proc", None),
        P("group", None, None, "proc", None),
        P("group", None, "proc", None),
        P("group", None, "proc", None),
    )
    out_specs = (
        P("group", None, None, "proc", None),
        P("group", None, "proc", None),
        P("group", None, None, "proc", None),
        P("group", None, "proc", None),
    )

    return jax.shard_map(per_device, mesh=mesh, in_specs=in_specs, out_specs=out_specs, check_vma=False)
```
